32 devices in a mesh: grp: 1, blk: 8 (over z, y), node: 4 (over x, core), pair: 1.
Axes of the slice: x: 2, y: 2, z: 4, core: 2. Of those that a mesh axis runs over, the one named last changes fastest.
Arguments:
- query: bfloat16 [4608, 1280], P(('grp', 'blk', 'node'), 'pair'), may hold values from -600 to 600
- key: bfloat16 [4608, 1280], P(('grp', 'blk', 'node'), 'pair'), may hold values from -25 to 25
- value: bfloat16 [4608, 1280], P(('grp', 'blk', 'node'), 'pair'), may hold values from -6 to 6
- out_weight: bfloat16 [1280, 1280], P('pair'), may hold values from -0.15625 to 0.15625
Outputs:
- mixed: bfloat16 [4608, 1280], P(('grp', 'blk', 'node', 'pair'))
The draws below stay inside these ranges and needn't reach their ends.
All inputs are finite; a program needn't handle non-finite values.
Results may differ from the reference program's by a relative error of at most 0.011.
Values may be sent and summed in bfloat16 or wider, within the bound.
A program may use at most 128 MiB of HBM per device.

```python
import math
import jax
import jax.numpy as jnp
from jax import lax

D = 1280
HEADS = 20
HD = 64
TOKENS = 4608


def key_rows(key):
    base = jnp.clip(jax.random.normal(jax.random.fold_in(key, 101), (TOKENS, D), jnp.float32), -4.5, 4.5)
    return base.astype(jnp.bfloat16)


def draw_key(key, part):
    return key_rows(key)


def draw_query(key, part):
    drawn = jax.random.normal(jax.random.fold_in(key, 105), (TOKENS, D), jnp.float32) * 2.5
    return jnp.clip(drawn, -12.0, 12.0).astype(jnp.bfloat16)


def block_levels(own_key, extent, shards, least, top_value):
    gain = 1.0
    for dim, shards_of in shards:
        steps = jax.random.uniform(jax.random.fold_in(jax.random.fold_in(own_key, 6), dim), (shards_of,), jnp.float32, least / len(shards), top_value / len(shards))
        gain = gain * jnp.repeat(jnp.exp(steps), extent[dim] // shards_of).reshape((-1,) + (1,) * (len(extent) - 1 - dim))
    return gain


def scatter_about(rng, shape, scale, reach, cuts=(), held_as=jnp.bfloat16):
    array = scale * jax.random.normal(rng, shape, jnp.float32)
    if cuts:
        array = array * block_levels(rng, shape, cuts, -0.22, 0.18)
    return jnp.clip(array, -reach, reach).astype(held_as)


def setup_inputs(seed: int = 0, part: int = 0) -> dict:
    keys = jax.random.split(jax.random.key(seed), 5)
    own_keys = jax.random.split(jax.random.fold_in(keys[4], part), 5)
    return {
        "query": draw_query(jax.random.fold_in(jax.random.fold_in(keys[4], part), 71), part),
        "key": draw_key(jax.random.fold_in(jax.random.fold_in(keys[4], part), 71), part),
        "value": scatter_about(own_keys[2], (TOKENS, D), 1.0, 6.0, ((0, 32),)),
        "out_weight": scatter_about(keys[3], (D, D), D ** -0.5, 0.15625),
    }


def reference(query, key, value, out_weight):
    scale = 1.0 / math.sqrt(HD)
    q_heads = query.reshape(TOKENS, HEADS, HD).transpose(1, 0, 2)
    k_heads = key.reshape(TOKENS, HEADS, HD).transpose(1, 0, 2)
    v_heads = value.reshape(TOKENS, HEADS, HD).transpose(1, 0, 2)

    def one_head(operands):
        q_one, k_one, v_one = operands
        scores = jnp.dot(q_one, k_one.T, preferred_element_type=jnp.float32) * scale
        peak = lax.optimization_barrier(jnp.max(scores, axis=1, keepdims=True))
        expo = jnp.exp(scores - peak)
        total = lax.optimization_barrier(jnp.sum(expo, axis=1, keepdims=True))
        return jnp.dot(expo.astype(jnp.bfloat16), v_one, preferred_element_type=jnp.float32) / total
    heads_out = lax.map(one_head, (q_heads, k_heads, v_heads))
    attn = heads_out.transpose(1, 0, 2).reshape(TOKENS, D).astype(jnp.bfloat16)
    return jnp.dot(attn, out_weight, preferred_element_type=jnp.float32).astype(jnp.bfloat16)
```

```python
import functools
import math

import jax
import jax.numpy as jnp
from jax import lax
from jax.experimental import pallas as pl
from jax.experimental.pallas import tpu as pltpu
from jax.sharding import PartitionSpec as P

HD = 64
WIDE = 2 * HD


def groups_of(blk, heads):
    return max(g for g in range(1, blk + 1) if blk % g == 0 and heads % g == 0)


def kernel(
    G, B, N,
    query_ref, key_ref, value_ref, weight_ref, mixed_ref,
    qp, kvp, kvz, qbuf, kvbuf, vbuf, qfull, peaks, accum, opack, oin, attn, weight,
    z_send, z_recv, q_send, q_recv, kv_send, kv_recv, o_send, o_recv, w_sem,
):
    H, R2, _ = qp.shape
    R = kvp.shape[1]
    hg = H // G
    PL = B // G
    inner = PL // N
    NS = kvbuf.shape[0]
    C = math.gcd(H, B)
    blk, node = lax.axis_index("blk"), lax.axis_index("node")
    z = blk // inner
    p = (blk % inner) * N + node
    bf, f32 = jnp.bfloat16, jnp.float32

    load_weight = pltpu.make_async_copy(weight_ref, weight, w_sem)
    load_weight.start()
    barrier = pltpu.get_barrier_semaphore()
    here = blk * N + node

    def greet(d, _):
        other = lax.rem(here + d, B)
        pl.semaphore_signal(
            barrier, inc=1, device_id={"blk": other // N, "node": lax.rem(other, N)},
            device_id_type=pl.DeviceIdType.MESH,
        )
        return 0

    lax.fori_loop(1, B, greet, 0)

    def peer(zz, pp):
        return {"blk": zz * inner + pp // N, "node": pp % N}

    def remote(src, dst, send, recv, zz, pp):
        return pltpu.make_async_remote_copy(
            src_ref=src, dst_ref=dst, send_sem=send, recv_sem=recv,
            device_id=peer(zz, pp), device_id_type=pl.DeviceIdType.MESH,
        )

    half = lax.broadcasted_iota(jnp.int32, (R2, WIDE), 1) < HD
    wide_half = lax.broadcasted_iota(jnp.int32, (R, WIDE), 1) < HD

    for pair in range(H // 2):
        columns = slice(pair * WIDE, (pair + 1) * WIDE)
        block = query_ref[:, columns].astype(f32)
        turned = pltpu.roll(block, HD, 1)
        qp[2 * pair] = jnp.where(half, block[:R2], turned[R2:]).astype(bf)
        qp[2 * pair + 1] = jnp.where(half, turned[:R2], block[R2:]).astype(bf)
    for pair in range(H // 2):
        columns = slice(pair * WIDE, (pair + 1) * WIDE)
        keys = key_ref[:, columns].astype(f32)
        values = value_ref[:, columns].astype(f32)
        kvp[2 * pair] = jnp.where(wide_half, keys, pltpu.roll(values, HD, 1)).astype(bf)
        kvp[2 * pair + 1] = jnp.where(wide_half, pltpu.roll(keys, HD, 1), values).astype(bf)

    pl.semaphore_wait(barrier, B - 1)

    def send_q(i, act):
        row = lax.rem((z + 1) * hg + i, H)
        zz = row // hg
        n = (row - zz * hg) * B + here
        pp = n // H
        u = n - pp * H
        mine = jnp.logical_and(zz == z, pp == p)

        @pl.when(jnp.logical_not(mine))
        def _():
            act(remote(qp.at[row], qbuf.at[u], q_send.at[row], q_recv.at[u], zz, pp))

        return mine, row, u

    def start_q(i, _):
        mine, row, u = send_q(i, lambda c: c.start())

        @pl.when(mine)
        def _():
            pltpu.make_async_copy(qp.at[row], qbuf.at[u], q_recv.at[u]).start()

        return 0

    lax.fori_loop(0, H, start_q, 0)

    def phase1(dz):
        g = lax.rem(z + dz, G)
        return remote(
            kvp.at[pl.ds(g * hg, hg)], kvz.at[dz - 1], z_send.at[dz - 1], z_recv.at[dz - 1], g, p
        )

    for dz in range(1, G):
        phase1(dz).start()

    def first(pp):
        return (pp * H) // B

    def last(pp):
        return (pp * H + H - 1) // B

    def kv_src(s, h):
        return kvp.at[z * hg + h] if s == 0 else kvz.at[s - 1, h]

    def share_kv(s, act):
        b = s * PL + p

        def one(dp, _):
            pp = lax.rem(p + dp, PL)
            for slot in range(NS):
                @pl.when(first(pp) + slot <= last(pp))
                def _():
                    act(remote(
                        kv_src(s, first(pp) + slot), kvbuf.at[slot, b],
                        kv_send.at[s, dp, slot], kv_recv.at[slot, b], z, pp,
                    ))
            return 0

        lax.fori_loop(1, PL, one, 0)

    def own_kv(s):
        b = s * PL + p
        for slot in range(NS):
            @pl.when(first(p) + slot <= last(p))
            def _():
                pltpu.make_async_copy(kv_src(s, first(p) + slot), kvbuf.at[slot, b], kv_recv.at[slot, b]).start()

    start = lambda c: c.start()
    share_kv(0, start)
    own_kv(0)

    scale = 1.0 / math.sqrt(HD)

    def take_q(u, _):
        pltpu.make_async_copy(qbuf.at[u], qbuf.at[u], q_recv.at[u]).wait()
        both = qbuf[u].astype(f32) * scale
        zero = jnp.zeros_like(both)
        qfull[u] = jnp.concatenate(
            [jnp.where(half, both, zero), jnp.where(half, pltpu.roll(both, HD, 1), zero)], axis=0
        ).astype(bf)
        return 0

    def take_kv(low, high):
        for slot in range(NS):
            @pl.when(first(p) + slot <= last(p))
            def _():
                def one(b, _):
                    pltpu.make_async_copy(kvbuf.at[slot, b], kvbuf.at[slot, b], kv_recv.at[slot, b]).wait()
                    vbuf[slot, b] = jnp.where(wide_half, jnp.ones((), bf), kvbuf[slot, b])
                    return 0
                lax.fori_loop(low * PL, high * PL, one, 0)

    def give(u, act):
        n = p * H + u
        h = n // B
        b = n - h * B
        zz, pp = b // PL, lax.rem(b, PL)
        mine = jnp.logical_and(zz == z, pp == p)
        row = z * hg + h

        @pl.when(jnp.logical_not(mine))
        def _():
            act(remote(opack.at[u], oin.at[row], o_send.at[u], o_recv.at[row], zz, pp))

        return mine, row

    def attend(low, high, t):
        slot = (p * H + t * C) // B - first(p)
        keys = kvbuf[slot, low * PL:high * PL].reshape((high - low) * PL * R, WIDE)
        values = vbuf[slot, low * PL:high * PL].reshape((high - low) * PL * R, WIDE)

        def product(c):
            return lax.dot_general(
                qfull[t * C + c], keys, (((1,), (1,)), ((), ())), preferred_element_type=f32
            )

        def soften(c, scores):
            u = t * C + c
            peak = jnp.max(scores, axis=1, keepdims=True)
            if low > 0:
                before = peaks[u]
                peak = jnp.maximum(before[:, :1], peak)
            expo = jnp.exp(scores - peak).astype(bf)
            total = jnp.dot(expo, values, preferred_element_type=f32)
            if low > 0:
                total = total + accum[u] * jnp.exp(before - peak)
            if high < G:
                peaks[u] = jnp.broadcast_to(peak, (R, WIDE))
                accum[u] = total
                return
            turned = pltpu.roll(total, HD, 1)
            opack[u] = jnp.where(
                half, turned[:R2] / total[:R2], total[R2:] / turned[R2:]
            ).astype(bf)

        scores = product(0)
        for c in range(C):
            ahead = product(c + 1) if c + 1 < C else None
            soften(c, scores)
            scores = ahead
        if high < G:
            return
        for i in range(C):
            u = t * C + i
            mine, row = give(u, start)

            @pl.when(mine)
            def _():
                pltpu.make_async_copy(opack.at[u], oin.at[row], o_recv.at[row]).start()

    def relay(s):
        if s < G:
            phase1(s).wait_recv()
            share_kv(s, start)
            own_kv(s)

    stages = [(s, s + 1) for s in range(min(G, 2))]
    stages += [(s, min(s + 2, G)) for s in range(2, G, 2)]
    turns = H // C
    relay(1)
    lax.fori_loop(0, H, take_q, 0)
    for low, high in stages:
        take_kv(low, high)

        def turn(t, _):
            attend(low, high, t)
            return 0

        if high == 2 and low == 1 and G > 3:
            lax.fori_loop(0, turns // 2, turn, 0)
            relay(3)
            lax.fori_loop(turns // 2, turns, turn, 0)
        else:
            lax.fori_loop(0, turns, turn, 0)
        if high == 1:
            relay(2)
        if high >= 2:
            for s in range(high + 2, min(high + 4, G)):
                relay(s)

    for dz in range(1, G):
        phase1(dz).wait_send()
    for s in range(G):
        share_kv(s, lambda c: c.wait_send())

    def end_q(i, _):
        send_q(i, lambda c: c.wait_send())
        return 0

    lax.fori_loop(0, H, end_q, 0)

    def end(u, _):
        give(u, lambda c: c.wait_send())
        pltpu.make_async_copy(oin.at[u], oin.at[u], o_recv.at[u]).wait()
        return 0

    load_weight.wait()
    lax.fori_loop(0, H, end, 0)
    for pair in range(H // 2):
        even, odd = oin[2 * pair].astype(f32), oin[2 * pair + 1].astype(f32)
        attn[:, pair * WIDE:(pair + 1) * WIDE] = jnp.concatenate(
            [
                jnp.where(half, even, pltpu.roll(odd, HD, 1)),
                jnp.where(half, pltpu.roll(even, HD, 1), odd),
            ],
            axis=0,
        ).astype(bf)
    mixed_ref[...] = jnp.dot(attn[...], weight[...], preferred_element_type=f32).astype(bf)


def chip_kernel(
    G, B, N,
    query_ref, key_ref, value_ref, weight_ref, mixed_ref,
    qin, kin, vin, qp, kvp, kv, qbuf, qfull, scored, expos, shift, peaks, accum, opack, oin, attn, weight,
    in_sem, kv_send, kv_recv, q_send, q_recv, s_send, c_send, c_recv, o_send, o_recv, w_sem,
):
    H, R2, _ = qp.shape
    R = kvp.shape[1]
    hg = H // G
    PL = B // G
    inner = PL // N
    C = PL // 2
    blk, node = lax.axis_index("blk"), lax.axis_index("node")
    z, y = blk // inner, blk % inner
    x, c = node // 2, node % 2
    bf, f32 = jnp.bfloat16, jnp.float32

    def column(r):
        return lax.rem(y + r // 2, 2), lax.rem(x + r % 2, 2)

    def at(dz, r, core=None):
        yy, xx = column(r)
        return {
            "blk": lax.rem(z + dz, G) * inner + yy,
            "node": xx * 2 + (c if core is None else core),
        }

    def main_row(dz, r):
        yy, xx = column(r)
        return lax.rem(z + dz, G) * hg + yy * 2 + xx

    def last_row(dz):
        return lax.rem(z + dz, G) * hg + C

    def remote(src, dst, send, recv, peer):
        return pltpu.make_async_remote_copy(
            src_ref=src, dst_ref=dst, send_sem=send, recv_sem=recv,
            device_id=peer, device_id_type=pl.DeviceIdType.MESH,
        )

    def arrived(ref, sem):
        pltpu.make_async_copy(ref, ref, sem).wait()

    loads = [
        pltpu.make_async_copy(ref, buf, in_sem.at[n])
        for n, (ref, buf) in enumerate(((key_ref, kin), (value_ref, vin), (query_ref, qin)))
    ]
    for load in loads:
        load.start()
    partner = at(0, 0, 1 - c)
    pairs = [(dz, r) for dz in range(G) for r in range(C) if dz or r]
    barrier = pltpu.get_barrier_semaphore()
    for peer in [partner] + [at(dz, r) for dz, r in pairs]:
        pl.semaphore_signal(barrier, inc=1, device_id=peer, device_id_type=pl.DeviceIdType.MESH)
    load_weight = pltpu.make_async_copy(weight_ref, weight, w_sem)
    load_weight.start()

    peaks[...] = jnp.full(peaks.shape, jnp.finfo(f32).min, f32)
    accum[...] = jnp.zeros(accum.shape, f32)
    scored[...] = jnp.full(scored.shape, -jnp.inf, f32)
    expos[...] = jnp.zeros(expos.shape, bf)
    shift[...] = jnp.ones(shift.shape, f32)
    half = lax.broadcasted_iota(jnp.int32, (R2, WIDE), 1) < HD
    wide_half = lax.broadcasted_iota(jnp.int32, (R, WIDE), 1) < HD

    loads[0].wait()
    loads[1].wait()
    for pair in range(H // 2):
        columns = slice(pair * WIDE, (pair + 1) * WIDE)
        keys = kin[:, columns].astype(f32)
        values = vin[:, columns].astype(f32)
        kvp[2 * pair] = jnp.where(wide_half, keys, pltpu.roll(values, HD, 1)).astype(bf)
        kvp[2 * pair + 1] = jnp.where(wide_half, pltpu.roll(keys, HD, 1), values).astype(bf)
    loads[2].wait()
    for pair in range(H // 2):
        columns = slice(pair * WIDE, (pair + 1) * WIDE)
        block = qin[:, columns].astype(f32)
        turned = pltpu.roll(block, HD, 1)
        qp[2 * pair] = jnp.where(half, block[:R2], turned[R2:]).astype(bf)
        qp[2 * pair + 1] = jnp.where(half, turned[:R2], block[R2:]).astype(bf)
    kv[0, 0, 0, 0] = kvp[main_row(0, 0)]
    kv[1, 0, 0, 0] = kvp[last_row(0)]
    qbuf[0, 0] = qp[main_row(0, 0)]
    qbuf[G, 0] = qp[last_row(0)]

    pl.semaphore_wait(barrier, len(pairs) + 1)

    def send_kv(dz, r):
        return remote(kvp.at[main_row(dz, r)], kv.at[0, dz, 0, r], kv_send.at[0], kv_recv.at[0, dz, r], at(dz, r))

    def send_q(dz, r):
        return remote(qp.at[main_row(dz, r)], qbuf.at[dz, r], q_send.at[0], q_recv.at[dz, r], at(dz, r))

    def share(s):
        for r in range(1, C):
            remote(kv.at[1, s, 0, 0], kv.at[1, s, 0, r], s_send, kv_recv.at[1, s, r], at(0, r)).start()

    for r in range(1, C):
        send_kv(0, r).start()
    share(0)
    for dz in range(1, G):
        remote(kvp.at[last_row(dz)], kv.at[1, dz, 0, 0], kv_send.at[1], kv_recv.at[1, dz, 0], at(dz, 0)).start()
    for dz in range(1, G):
        remote(qp.at[last_row(dz)], qbuf.at[G, dz], q_send.at[1], q_recv.at[G, dz], at(dz, 0)).start()
    for r in range(1, C):
        send_q(0, r).start()
    for dz in range(1, G):
        for r in range(C):
            send_kv(dz, r).start()
    for dz in range(1, G):
        for r in range(C):
            send_q(dz, r).start()

    def cross(kind, s):
        for r in range(C):
            if not isinstance(s, int) or s or r:
                arrived(kv.at[kind, s, 0, r], kv_recv.at[kind, s, r])
        remote(kv.at[kind, s, 0], kv.at[kind, s, 1], c_send.at[kind], c_recv.at[kind, s], partner).start()

    def spread(s):
        arrived(kv.at[1, s, 0, 0], kv_recv.at[1, s, 0])
        share(s)

    def cross_shared(s):
        for r in range(1, C):
            arrived(kv.at[1, s, 0, r], kv_recv.at[1, s, r])
        remote(kv.at[1, s, 0], kv.at[1, s, 1], c_send.at[1], c_recv.at[1, s], partner).start()

    scale = 1.0 / math.sqrt(HD)

    def widen(u, b):
        both = qbuf[u, b].astype(f32) * scale
        zero = jnp.zeros_like(both)
        qfull[b] = jnp.concatenate(
            [jnp.where(half, both, zero), jnp.where(half, pltpu.roll(both, HD, 1), zero)], axis=0
        ).astype(bf)

    def give(u, b):
        last = u == G
        plane = lax.rem(z + G - jnp.where(last, b, u), G)
        yy, xx = column(b)
        row = jnp.where(last, last_row(0), main_row(0, 0))
        return remote(
            opack.at[u, b], oin.at[row], o_send.at[u], o_recv.at[row],
            {
                "blk": plane * inner + jnp.where(last, y, yy),
                "node": jnp.where(last, x, xx) * 2 + c,
            },
        )

    PART = C // 2
    M = PART * R
    first_half = lax.broadcasted_iota(jnp.int32, (PL * R, WIDE), 1) < HD

    def unit(t):
        t = jnp.maximum(t, 0)
        return lax.rem(t // G + G, G + 1), t % G

    def keys_of(u, s):
        return kv[u // G, s].reshape(PL * R, WIDE)

    def values_of(u, s):
        return jnp.where(first_half, jnp.ones((), bf), keys_of(u, s))

    def product(part, keys):
        return lax.dot_general(
            qfull[part * PART:(part + 1) * PART].reshape(M, WIDE), keys,
            (((1,), (1,)), ((), ())), preferred_element_type=f32,
        )

    def soften(part, u):
        rows = slice(part * M, (part + 1) * M)
        scores = scored[part]
        before = peaks[u, rows]
        peak = jnp.maximum(before, jnp.max(scores, axis=1, keepdims=True))
        peaks[u, rows] = peak
        shift[part] = jnp.exp(before - peak)
        expos[part] = jnp.exp(scores - peak[:, :1]).astype(bf)

    def gather(part, u, values):
        rows = slice(part * M, (part + 1) * M)
        total = jnp.dot(expos[part], values, preferred_element_type=f32)
        accum[u, rows] = total + accum[u, rows] * shift[part]

    def finish(u, b):
        total = accum[u, b * R:(b + 1) * R]
        turned = pltpu.roll(total, HD, 1)
        opack[u, b] = jnp.where(
            half, turned[:R2] / total[:R2], total[R2:] / turned[R2:]
        ).astype(bf)
        if b:
            give(u, b).start()
        else:
            stays = jnp.logical_or(u == 0, u == G)

            @pl.when(stays)
            def _():
                oin[jnp.where(u == G, last_row(0), main_row(0, 0))] = opack[u, 0]

            @pl.when(jnp.logical_not(stays))
            def _():
                give(u, 0).start()

    cross(0, 0)
    cross_shared(0)
    for s in range(1, G):
        spread(s)
    for s in range(1, G):
        cross_shared(s)

    def tick(t, _):
        u, s = unit(t)
        v, w = unit(t - 1)
        for n in range(1, G):
            @pl.when(t == G + n)
            def _():
                cross(0, n)

        @pl.when(jnp.logical_or(u == 0, u == G))
        def _():
            arrived(kv.at[u // G, s, 1], c_recv.at[u // G, s])

        @pl.when(s == 0)
        def _():
            for b in range(C):
                @pl.when(jnp.logical_or(b > 0, jnp.logical_and(u > 0, u < G)))
                def _():
                    arrived(qbuf.at[u, b], q_recv.at[u, b])
                widen(u, b)

        keys, values = keys_of(u, s), values_of(v, w)
        gather(0, v, values)
        scored[0] = product(0, keys)
        soften(1, v)
        scored[1] = product(1, keys)
        gather(1, v, values)
        soften(0, u)

        @pl.when(jnp.logical_and(t > 0, w == G - 1))
        def _():
            for b in range(C):
                finish(v, b)

        return 0

    units = (G + 1) * G
    lax.fori_loop(0, units, tick, 0)
    v, w = unit(units - 1)
    values = values_of(v, w)
    gather(0, v, values)
    soften(1, v)
    for b in range(PART):
        finish(v, b)
    gather(1, v, values)
    for b in range(PART, C):
        finish(v, b)

    arrived(kvp.at[0:len(pairs)], kv_send.at[0])
    arrived(kvp.at[0:G - 1], kv_send.at[1])
    arrived(qp.at[0:len(pairs)], q_send.at[0])
    arrived(qp.at[0:G - 1], q_send.at[1])
    arrived(kvp.at[0:G * (C - 1)], s_send)
    for kind in range(2):
        arrived(kvp.at[0:G * C], c_send.at[kind])
    for u in range(G + 1):
        arrived(qp.at[0:C - (1 if u in (0, G) else 0)], o_send.at[u])
    for dz, r in pairs:
        arrived(oin.at[main_row(dz, r)], o_recv.at[main_row(dz, r)])
    for dz in range(1, G):
        arrived(oin.at[last_row(dz)], o_recv.at[last_row(dz)])
    load_weight.wait()
    for pair in range(H // 2):
        even, odd = oin[2 * pair].astype(f32), oin[2 * pair + 1].astype(f32)
        attn[:, pair * WIDE:(pair + 1) * WIDE] = jnp.concatenate(
            [
                jnp.where(half, even, pltpu.roll(odd, HD, 1)),
                jnp.where(half, pltpu.roll(even, HD, 1), odd),
            ],
            axis=0,
        ).astype(bf)
    mixed_ref[...] = jnp.dot(attn[...], weight[...], preferred_element_type=f32).astype(bf)


def chip_call(query, key, value, out_weight, G, B, N):
    R, features = query.shape
    H = features // HD
    R2 = R // 2
    C = B // G // 2
    dma = pltpu.SemaphoreType.DMA
    bf, f32 = jnp.bfloat16, jnp.float32
    anywhere = pl.BlockSpec(memory_space=pl.ANY)
    return pl.pallas_call(
        functools.partial(chip_kernel, G, B, N),
        out_shape=jax.ShapeDtypeStruct((R, out_weight.shape[1]), bf),
        in_specs=[anywhere] * 4,
        out_specs=pl.BlockSpec(memory_space=pltpu.VMEM),
        scratch_shapes=[
            pltpu.VMEM((R, features), bf),
            pltpu.VMEM((R, features), bf),
            pltpu.VMEM((R, features), bf),
            pltpu.VMEM((H, R2, WIDE), bf),
            pltpu.VMEM((H, R, WIDE), bf),
            pltpu.VMEM((2, G, 2, C, R, WIDE), bf),
            pltpu.VMEM((G + 1, C, R2, WIDE), bf),
            pltpu.VMEM((C, R, WIDE), bf),
            pltpu.VMEM((2, C // 2 * R, B // G * R), f32),
            pltpu.VMEM((2, C // 2 * R, B // G * R), bf),
            pltpu.VMEM((2, C // 2 * R, WIDE), f32),
            pltpu.VMEM((G + 1, C * R, WIDE), f32),
            pltpu.VMEM((G + 1, C * R, WIDE), f32),
            pltpu.VMEM((G + 1, C, R2, WIDE), bf),
            pltpu.VMEM((H, R2, WIDE), bf),
            pltpu.VMEM((R, features), bf),
            pltpu.VMEM(out_weight.shape, bf),
            dma((3,)),
            dma((2,)), dma((2, G, C)),
            dma((2,)), dma((G + 1, C)),
            dma(()),
            dma((2,)), dma((2, G)),
            dma((G + 1,)), dma((H,)),
            dma(()),
        ],
        compiler_params=pltpu.CompilerParams(
            collective_id=0, has_side_effects=True, vmem_limit_bytes=60 * 1024 * 1024
        ),
        name="attention",
    )(query, key, value, out_weight)


def per_device(query, key, value, out_weight):
    R, features = query.shape
    H = features // HD
    R2 = R // 2
    nblk, N = lax.axis_size("blk"), lax.axis_size("node")
    B = nblk * N
    G = groups_of(nblk, H)
    hg = H // G
    NS = (H + B - 2) // B + 1
    dma = pltpu.SemaphoreType.DMA
    bf, f32 = jnp.bfloat16, jnp.float32
    vmem = pl.BlockSpec(memory_space=pltpu.VMEM)
    if G == N and nblk == 2 * G and hg == G + 1 and R % 16 == 0:
        mixed = chip_call(query, key, value, out_weight, G, B, N)
        return lax.psum_scatter(mixed, "pair", scatter_dimension=0, tiled=True)
    mixed = pl.pallas_call(
        functools.partial(kernel, G, B, N),
        out_shape=jax.ShapeDtypeStruct((R, out_weight.shape[1]), bf),
        in_specs=[vmem, vmem, vmem, pl.BlockSpec(memory_space=pl.ANY)],
        out_specs=vmem,
        scratch_shapes=[
            pltpu.VMEM((H, R2, WIDE), bf),
            pltpu.VMEM((H, R, WIDE), bf),
            pltpu.VMEM((max(G - 1, 1), hg, R, WIDE), bf),
            pltpu.VMEM((H, R2, WIDE), bf),
            pltpu.VMEM((NS, B, R, WIDE), bf),
            pltpu.VMEM((NS, B, R, WIDE), bf),
            pltpu.VMEM((H, R, WIDE), bf),
            pltpu.VMEM((H, R, WIDE), f32),
            pltpu.VMEM((H, R, WIDE), f32),
            pltpu.VMEM((H, R2, WIDE), bf),
            pltpu.VMEM((H, R2, WIDE), bf),
            pltpu.VMEM((R, features), bf),
            pltpu.VMEM(out_weight.shape, bf),
            dma((max(G - 1, 1),)),
            dma((max(G - 1, 1),)),
            dma((H,)),
            dma((H,)),
            dma((G, B // G, NS)),
            dma((NS, B)),
            dma((H,)),
            dma((H,)),
            dma(()),
        ],
        compiler_params=pltpu.CompilerParams(
            collective_id=0, has_side_effects=True, vmem_limit_bytes=60 * 1024 * 1024
        ),
        name="attention",
    )(query, key, value, out_weight)
    return lax.psum_scatter(mixed, "pair", scatter_dimension=0, tiled=True)


def solution(mesh):
    in_specs = (
        P(("grp", "blk", "node"), "pair"),
        P(("grp", "blk", "node"), "pair"),
        P(("grp", "blk", "node"), "pair"),
        P("pair", None),
    )
    out_specs = P(("grp", "blk", "node", "pair"), None)
    return jax.shard_map(
        per_device, mesh=mesh, in_specs=in_specs, out_specs=out_specs, check_vma=False
    )
```

```python
import functools
import math

import jax
import jax.numpy as jnp
from jax import lax
from jax.experimental import pallas as pl
from jax.experimental.pallas import tpu as pltpu
from jax.sharding import PartitionSpec as P

HD = 64
WIDE = 2 * HD


def groups_of(blk, heads):
    return max(g for g in range(1, blk + 1) if blk % g == 0 and heads % g == 0)


def kernel(
    G, B, N,
    query_ref, key_ref, value_ref, weight_ref, mixed_ref,
    qp, kvp, kvz, qbuf, kvbuf, vbuf, qfull, peaks, accum, opack, oin, attn, weight,
    z_send, z_recv, q_send, q_recv, kv_send, kv_recv, o_send, o_recv, w_sem,
):
    H, R2, _ = qp.shape
    R = kvp.shape[1]
    hg = H // G
    PL = B // G
    inner = PL // N
    NS = kvbuf.shape[0]
    C = math.gcd(H, B)
    blk, node = lax.axis_index("blk"), lax.axis_index("node")
    z = blk // inner
    p = (blk % inner) * N + node
    bf, f32 = jnp.bfloat16, jnp.float32

    load_weight = pltpu.make_async_copy(weight_ref, weight, w_sem)
    load_weight.start()
    barrier = pltpu.get_barrier_semaphore()
    here = blk * N + node

    def greet(d, _):
        other = lax.rem(here + d, B)
        pl.semaphore_signal(
            barrier, inc=1, device_id={"blk": other // N, "node": lax.rem(other, N)},
            device_id_type=pl.DeviceIdType.MESH,
        )
        return 0

    lax.fori_loop(1, B, greet, 0)

    def peer(zz, pp):
        return {"blk": zz * inner + pp // N, "node": pp % N}

    def remote(src, dst, send, recv, zz, pp):
        return pltpu.make_async_remote_copy(
            src_ref=src, dst_ref=dst, send_sem=send, recv_sem=recv,
            device_id=peer(zz, pp), device_id_type=pl.DeviceIdType.MESH,
        )

    half = lax.broadcasted_iota(jnp.int32, (R2, WIDE), 1) < HD
    wide_half = lax.broadcasted_iota(jnp.int32, (R, WIDE), 1) < HD

    for pair in range(H // 2):
        columns = slice(pair * WIDE, (pair + 1) * WIDE)
        block = query_ref[:, columns].astype(f32)
        turned = pltpu.roll(block, HD, 1)
        qp[2 * pair] = jnp.where(half, block[:R2], turned[R2:]).astype(bf)
        qp[2 * pair + 1] = jnp.where(half, turned[:R2], block[R2:]).astype(bf)
    for pair in range(H // 2):
        columns = slice(pair * WIDE, (pair + 1) * WIDE)
        keys = key_ref[:, columns].astype(f32)
        values = value_ref[:, columns].astype(f32)
        kvp[2 * pair] = jnp.where(wide_half, keys, pltpu.roll(values, HD, 1)).astype(bf)
        kvp[2 * pair + 1] = jnp.where(wide_half, pltpu.roll(keys, HD, 1), values).astype(bf)

    pl.semaphore_wait(barrier, B - 1)

    def send_q(i, act):
        row = lax.rem((z + 1) * hg + i, H)
        zz = row // hg
        n = (row - zz * hg) * B + here
        pp = n // H
        u = n - pp * H
        mine = jnp.logical_and(zz == z, pp == p)

        @pl.when(jnp.logical_not(mine))
        def _():
            act(remote(qp.at[row], qbuf.at[u], q_send.at[row], q_recv.at[u], zz, pp))

        return mine, row, u

    def start_q(i, _):
        mine, row, u = send_q(i, lambda c: c.start())

        @pl.when(mine)
        def _():
            pltpu.make_async_copy(qp.at[row], qbuf.at[u], q_recv.at[u]).start()

        return 0

    lax.fori_loop(0, H, start_q, 0)

    def phase1(dz):
        g = lax.rem(z + dz, G)
        return remote(
            kvp.at[pl.ds(g * hg, hg)], kvz.at[dz - 1], z_send.at[dz - 1], z_recv.at[dz - 1], g, p
        )

    for dz in range(1, G):
        phase1(dz).start()

    def first(pp):
        return (pp * H) // B

    def last(pp):
        return (pp * H + H - 1) // B

    def kv_src(s, h):
        return kvp.at[z * hg + h] if s == 0 else kvz.at[s - 1, h]

    def share_kv(s, act):
        b = s * PL + p

        def one(dp, _):
            pp = lax.rem(p + dp, PL)
            for slot in range(NS):
                @pl.when(first(pp) + slot <= last(pp))
                def _():
                    act(remote(
                        kv_src(s, first(pp) + slot), kvbuf.at[slot, b],
                        kv_send.at[s, dp, slot], kv_recv.at[slot, b], z, pp,
                    ))
            return 0

        lax.fori_loop(1, PL, one, 0)

    def own_kv(s):
        b = s * PL + p
        for slot in range(NS):
            @pl.when(first(p) + slot <= last(p))
            def _():
                pltpu.make_async_copy(kv_src(s, first(p) + slot), kvbuf.at[slot, b], kv_recv.at[slot, b]).start()

    start = lambda c: c.start()
    share_kv(0, start)
    own_kv(0)

    scale = 1.0 / math.sqrt(HD)

    def take_q(u, _):
        pltpu.make_async_copy(qbuf.at[u], qbuf.at[u], q_recv.at[u]).wait()
        both = qbuf[u].astype(f32) * scale
        zero = jnp.zeros_like(both)
        qfull[u] = jnp.concatenate(
            [jnp.where(half, both, zero), jnp.where(half, pltpu.roll(both, HD, 1), zero)], axis=0
        ).astype(bf)
        return 0

    def take_kv(low, high):
        for slot in range(NS):
            @pl.when(first(p) + slot <= last(p))
            def _():
                def one(b, _):
                    pltpu.make_async_copy(kvbuf.at[slot, b], kvbuf.at[slot, b], kv_recv.at[slot, b]).wait()
                    vbuf[slot, b] = jnp.where(wide_half, jnp.ones((), bf), kvbuf[slot, b])
                    return 0
                lax.fori_loop(low * PL, high * PL, one, 0)

    def give(u, act):
        n = p * H + u
        h = n // B
        b = n - h * B
        zz, pp = b // PL, lax.rem(b, PL)
        mine = jnp.logical_and(zz == z, pp == p)
        row = z * hg + h

        @pl.when(jnp.logical_not(mine))
        def _():
            act(remote(opack.at[u], oin.at[row], o_send.at[u], o_recv.at[row], zz, pp))

        return mine, row

    def attend(low, high, t):
        slot = (p * H + t * C) // B - first(p)
        keys = kvbuf[slot, low * PL:high * PL].reshape((high - low) * PL * R, WIDE)
        values = vbuf[slot, low * PL:high * PL].reshape((high - low) * PL * R, WIDE)

        def product(c):
            return lax.dot_general(
                qfull[t * C + c], keys, (((1,), (1,)), ((), ())), preferred_element_type=f32
            )

        def soften(c, scores):
            u = t * C + c
            peak = jnp.max(scores, axis=1, keepdims=True)
            if low > 0:
                before = peaks[u]
                peak = jnp.maximum(before[:, :1], peak)
            expo = jnp.exp(scores - peak).astype(bf)
            total = jnp.dot(expo, values, preferred_element_type=f32)
            if low > 0:
                total = total + accum[u] * jnp.exp(before - peak)
            if high < G:
                peaks[u] = jnp.broadcast_to(peak, (R, WIDE))
                accum[u] = total
                return
            turned = pltpu.roll(total, HD, 1)
            opack[u] = jnp.where(
                half, turned[:R2] / total[:R2], total[R2:] / turned[R2:]
            ).astype(bf)

        scores = product(0)
        for c in range(C):
            ahead = product(c + 1) if c + 1 < C else None
            soften(c, scores)
            scores = ahead
        if high < G:
            return
        for i in range(C):
            u = t * C + i
            mine, row = give(u, start)

            @pl.when(mine)
            def _():
                pltpu.make_async_copy(opack.at[u], oin.at[row], o_recv.at[row]).start()

    def relay(s):
        if s < G:
            phase1(s).wait_recv()
            share_kv(s, start)
            own_kv(s)

    stages = [(s, s + 1) for s in range(min(G, 2))]
    stages += [(s, min(s + 2, G)) for s in range(2, G, 2)]
    turns = H // C
    relay(1)
    lax.fori_loop(0, H, take_q, 0)
    for low, high in stages:
        take_kv(low, high)

        def turn(t, _):
            attend(low, high, t)
            return 0

        if high == 2 and low == 1 and G > 3:
            lax.fori_loop(0, turns // 2, turn, 0)
            relay(3)
            lax.fori_loop(turns // 2, turns, turn, 0)
        else:
            lax.fori_loop(0, turns, turn, 0)
        if high == 1:
            relay(2)
        if high >= 2:
            for s in range(high + 2, min(high + 4, G)):
                relay(s)

    for dz in range(1, G):
        phase1(dz).wait_send()
    for s in range(G):
        share_kv(s, lambda c: c.wait_send())

    def end_q(i, _):
        send_q(i, lambda c: c.wait_send())
        return 0

    lax.fori_loop(0, H, end_q, 0)

    def end(u, _):
        give(u, lambda c: c.wait_send())
        pltpu.make_async_copy(oin.at[u], oin.at[u], o_recv.at[u]).wait()
        return 0

    load_weight.wait()
    lax.fori_loop(0, H, end, 0)
    for pair in range(H // 2):
        even, odd = oin[2 * pair].astype(f32), oin[2 * pair + 1].astype(f32)
        attn[:, pair * WIDE:(pair + 1) * WIDE] = jnp.concatenate(
            [
                jnp.where(half, even, pltpu.roll(odd, HD, 1)),
                jnp.where(half, pltpu.roll(even, HD, 1), odd),
            ],
            axis=0,
        ).astype(bf)
    mixed_ref[...] = jnp.dot(attn[...], weight[...], preferred_element_type=f32).astype(bf)


def chip_kernel(
    G, B, N,
    query_ref, key_ref, value_ref, weight_ref, mixed_ref,
    qin, kin, vin, qp, kvp, kv, qbuf, qfull, scored, expos, shift, peaks, accum, opack, oin, attn, weight,
    in_sem, kv_send, kv_recv, q_send, q_recv, s_send, c_send, c_recv, o_send, o_recv, w_sem,
):
    H, R2, _ = qp.shape
    R = kvp.shape[1]
    hg = H // G
    PL = B // G
    inner = PL // N
    C = PL // 2
    blk, node = lax.axis_index("blk"), lax.axis_index("node")
    z, y = blk // inner, blk % inner
    x, c = node // 2, node % 2
    bf, f32 = jnp.bfloat16, jnp.float32

    def column(r):
        return lax.rem(y + r // 2, 2), lax.rem(x + r % 2, 2)

    def at(dz, r, core=None):
        yy, xx = column(r)
        return {
            "blk": lax.rem(z + dz, G) * inner + yy,
            "node": xx * 2 + (c if core is None else core),
        }

    def main_row(dz, r):
        yy, xx = column(r)
        return lax.rem(z + dz, G) * hg + yy * 2 + xx

    def last_row(dz):
        return lax.rem(z + dz, G) * hg + C

    def remote(src, dst, send, recv, peer):
        return pltpu.make_async_remote_copy(
            src_ref=src, dst_ref=dst, send_sem=send, recv_sem=recv,
            device_id=peer, device_id_type=pl.DeviceIdType.MESH,
        )

    def arrived(ref, sem):
        pltpu.make_async_copy(ref, ref, sem).wait()

    loads = [
        pltpu.make_async_copy(ref, buf, in_sem.at[n])
        for n, (ref, buf) in enumerate(((key_ref, kin), (value_ref, vin), (query_ref, qin)))
    ]
    for load in loads:
        load.start()
    partner = at(0, 0, 1 - c)
    pairs = [(dz, r) for dz in range(G) for r in range(C) if dz or r]
    barrier = pltpu.get_barrier_semaphore()
    for peer in [partner] + [at(dz, r) for dz, r in pairs]:
        pl.semaphore_signal(barrier, inc=1, device_id=peer, device_id_type=pl.DeviceIdType.MESH)
    load_weight = pltpu.make_async_copy(weight_ref, weight, w_sem)
    load_weight.start()

    peaks[...] = jnp.full(peaks.shape, jnp.finfo(f32).min, f32)
    accum[...] = jnp.zeros(accum.shape, f32)
    scored[...] = jnp.full(scored.shape, -jnp.inf, f32)
    expos[...] = jnp.zeros(expos.shape, bf)
    shift[...] = jnp.ones(shift.shape, f32)
    half = lax.broadcasted_iota(jnp.int32, (R2, WIDE), 1) < HD
    wide_half = lax.broadcasted_iota(jnp.int32, (R, WIDE), 1) < HD

    loads[0].wait()
    loads[1].wait()
    for pair in range(H // 2):
        columns = slice(pair * WIDE, (pair + 1) * WIDE)
        keys = kin[:, columns].astype(f32)
        values = vin[:, columns].astype(f32)
        kvp[2 * pair] = jnp.where(wide_half, keys, pltpu.roll(values, HD, 1)).astype(bf)
        kvp[2 * pair + 1] = jnp.where(wide_half, pltpu.roll(keys, HD, 1), values).astype(bf)
    loads[2].wait()
    for pair in range(H // 2):
        columns = slice(pair * WIDE, (pair + 1) * WIDE)
        block = qin[:, columns].astype(f32)
        turned = pltpu.roll(block, HD, 1)
        qp[2 * pair] = jnp.where(half, block[:R2], turned[R2:]).astype(bf)
        qp[2 * pair + 1] = jnp.where(half, turned[:R2], block[R2:]).astype(bf)
    kv[0, 0, 0, 0] = kvp[main_row(0, 0)]
    kv[1, 0, 0, 0] = kvp[last_row(0)]
    qbuf[0, 0] = qp[main_row(0, 0)]
    qbuf[G, 0] = qp[last_row(0)]

    pl.semaphore_wait(barrier, len(pairs) + 1)

    def send_kv(dz, r):
        return remote(kvp.at[main_row(dz, r)], kv.at[0, dz, 0, r], kv_send.at[0], kv_recv.at[0, dz, r], at(dz, r))

    def send_q(dz, r):
        return remote(qp.at[main_row(dz, r)], qbuf.at[dz, r], q_send.at[0], q_recv.at[dz, r], at(dz, r))

    def share(s):
        for r in range(1, C):
            remote(kv.at[1, s, 0, 0], kv.at[1, s, 0, r], s_send, kv_recv.at[1, s, r], at(0, r)).start()

    for r in range(1, C):
        send_kv(0, r).start()
    for r in range(1, C):
        send_q(0, r).start()
    share(0)
    for dz in range(1, G):
        for r in range(C):
            send_q(dz, r).start()
    for dz in range(1, G):
        remote(qp.at[last_row(dz)], qbuf.at[G, dz], q_send.at[1], q_recv.at[G, dz], at(dz, 0)).start()
    def send_near():
        for dz in range(1, G, 2):
            for r in range(C):
                send_kv(dz, r).start()

    def send_shared():
        for dz in range(1, G):
            remote(kvp.at[last_row(dz)], kv.at[1, dz, 0, 0], kv_send.at[1], kv_recv.at[1, dz, 0], at(dz, 0)).start()

    def send_far():
        for dz in range(2, G, 2):
            for r in range(C):
                send_kv(dz, r).start()

    def cross(kind, s):
        for r in range(1 if kind or not s else 0, C):
            arrived(kv.at[kind, s, 0, r], kv_recv.at[kind, s, r])
        remote(kv.at[kind, s, 0], kv.at[kind, s, 1], c_send.at[kind], c_recv.at[kind, s], partner).start()

    def spread(s):
        arrived(kv.at[1, s, 0, 0], kv_recv.at[1, s, 0])
        share(s)

    scale = 1.0 / math.sqrt(HD)

    def widen(u, b):
        both = qbuf[u, b].astype(f32) * scale
        zero = jnp.zeros_like(both)
        qfull[u, b] = jnp.concatenate(
            [jnp.where(half, both, zero), jnp.where(half, pltpu.roll(both, HD, 1), zero)], axis=0
        ).astype(bf)

    def give(u, b):
        last = u == G
        plane = lax.rem(z + G - jnp.where(last, b, u), G)
        yy, xx = column(b)
        row = jnp.where(last, last_row(0), main_row(0, 0))
        return remote(
            opack.at[u, b], oin.at[row], o_send.at[u], o_recv.at[row],
            {
                "blk": plane * inner + jnp.where(last, y, yy),
                "node": jnp.where(last, x, xx) * 2 + c,
            },
        )

    PART = C // 2
    M = PART * R
    first_half = lax.broadcasted_iota(jnp.int32, (PL * R, WIDE), 1) < HD

    planes_order = [0] + list(range(1, G, 2)) + list(range(2, G, 2))
    order = [0] + list(range(1, G, 2)) + [G] + list(range(2, G, 2))
    MID = order.index(G)

    def pick(index, values):
        found = values[-1]
        for n, value in enumerate(values[:-1]):
            found = jnp.where(index == n, value, found)
        return found

    def unit(t):
        t = jnp.maximum(t, 0)
        k, m = t // G, t % G
        late = pick(m, list(range(2, G, 2)) + list(range(1, G, 2)) + [0])
        u = jnp.where(k == MID, G, jnp.where(k == G, late, m))
        s = jnp.where(k == MID, pick(m, planes_order), pick(k, order))
        return k, u, s

    def keys_of(u, s):
        return kv[u // G, s].reshape(PL * R, WIDE)

    def values_of(u, s):
        return jnp.where(first_half, jnp.ones((), bf), keys_of(u, s))

    def product(part, u, keys):
        return lax.dot_general(
            qfull[u, part * PART:(part + 1) * PART].reshape(M, WIDE), keys,
            (((1,), (1,)), ((), ())), preferred_element_type=f32,
        )

    def soften(part, u):
        rows = slice(part * M, (part + 1) * M)
        scores = scored[part]
        before = peaks[u, rows]
        peak = jnp.maximum(before, jnp.max(scores, axis=1, keepdims=True))
        peaks[u, rows] = peak
        shift[part] = jnp.exp(before - peak)
        expos[part] = jnp.exp(scores - peak[:, :1]).astype(bf)

    def gather(part, u, values):
        rows = slice(part * M, (part + 1) * M)
        total = jnp.dot(expos[part], values, preferred_element_type=f32)
        accum[u, rows] = total + accum[u, rows] * shift[part]

    def divide(u, b):
        total = accum[u, b * R:(b + 1) * R]
        turned = pltpu.roll(total, HD, 1)
        above = jnp.where(half, turned[:R2], total[R2:])
        below = jnp.where(half, total[:R2], turned[R2:])
        opack[u, b] = (above / below).astype(bf)

    def deliver(u, b):
        if b:
            give(u, b).start()
            return
        stays = jnp.logical_or(u == 0, u == G)

        @pl.when(stays)
        def _():
            oin[jnp.where(u == G, last_row(0), main_row(0, 0))] = opack[u, 0]

        @pl.when(jnp.logical_not(stays))
        def _():
            give(u, 0).start()

    inside = jnp.logical_and(z > 0, z < G - 1)

    @pl.when(inside)
    def _():
        send_near()
        send_shared()
        send_far()

    cross(0, 0)

    @pl.when(jnp.logical_not(inside))
    def _():
        send_near()

    stages = {4: send_shared, 8: send_far}
    steps = {
        3: [(cross, 0, 1)],
        6: [(cross, 0, 3), (cross, 1, 0)],
        8: [(spread, 1)],
        9: [(spread, 3)],
        11: [(spread, 2)],
        12: [(cross, 1, 1)],
        13: [(cross, 1, 3)],
        14: [(cross, 1, 2)],
        15: [(cross, 0, 2)],
    }

    def tick(t, _, ending=False):
        k, u, s = unit(t)
        j, v, w = unit(t - 1)
        if not ending:
            for n, stage in stages.items():
                pl.when(jnp.logical_and(t == n, jnp.logical_not(inside)))(stage)
            for n, step in steps.items():
                @pl.when(t == n)
                def _():
                    for act, *where in step:
                        act(*where)

            @pl.when(jnp.logical_or(k == MID, t % G == 0))
            def _():
                arrived(kv.at[u // G, s, 1], c_recv.at[u // G, s])

            @pl.when(jnp.logical_or(k == 0, t == MID * G))
            def _():
                for b in range(C):
                    @pl.when(jnp.logical_or(b > 0, jnp.logical_and(u > 0, u < G)))
                    def _():
                        arrived(qbuf.at[u, b], q_recv.at[u, b])
                    widen(u, b)

        keys, values = keys_of(u, s), values_of(v, w)
        gather(0, v, values)
        scored[0] = product(0, u, keys)
        soften(1, v)
        scored[1] = product(1, u, keys)
        gather(1, v, values)
        if ending:
            for b in range(C):
                divide(v, b)
        soften(0, u)
        if ending:
            for b in range(C):
                deliver(v, b)
            return 0

        @pl.when(t == (MID + 1) * G)
        def _():
            for b in range(C):
                divide(v, b)
                deliver(v, b)

        return 0

    units = (G + 1) * G
    lax.fori_loop(0, units - G + 1, tick, 0)
    lax.fori_loop(units - G + 1, units, functools.partial(tick, ending=True), 0)
    j, v, w = unit(units - 1)
    values = values_of(v, w)
    gather(0, v, values)
    soften(1, v)
    for b in range(PART):
        divide(v, b)
        deliver(v, b)
    gather(1, v, values)
    for b in range(PART, C):
        divide(v, b)
        deliver(v, b)

    load_weight.wait()
    for dz in range(1, G):
        arrived(oin.at[last_row(dz)], o_recv.at[last_row(dz)])
    for dz, r in pairs:
        arrived(oin.at[main_row(dz, r)], o_recv.at[main_row(dz, r)])
    for pair in range(H // 2):
        even, odd = oin[2 * pair].astype(f32), oin[2 * pair + 1].astype(f32)
        attn[:, pair * WIDE:(pair + 1) * WIDE] = jnp.concatenate(
            [
                jnp.where(half, even, pltpu.roll(odd, HD, 1)),
                jnp.where(half, pltpu.roll(even, HD, 1), odd),
            ],
            axis=0,
        ).astype(bf)
    mixed_ref[...] = jnp.dot(attn[...], weight[...], preferred_element_type=f32).astype(bf)

    arrived(kvp.at[0:len(pairs)], kv_send.at[0])
    arrived(kvp.at[0:G - 1], kv_send.at[1])
    arrived(qp.at[0:len(pairs)], q_send.at[0])
    arrived(qp.at[0:G - 1], q_send.at[1])
    arrived(kvp.at[0:G * (C - 1)], s_send)
    for kind in range(2):
        arrived(kvp.at[0:G * C], c_send.at[kind])
    for u in range(G + 1):
        arrived(qp.at[0:C - (1 if u in (0, G) else 0)], o_send.at[u])


def chip_call(query, key, value, out_weight, G, B, N):
    R, features = query.shape
    H = features // HD
    R2 = R // 2
    C = B // G // 2
    dma = pltpu.SemaphoreType.DMA
    bf, f32 = jnp.bfloat16, jnp.float32
    anywhere = pl.BlockSpec(memory_space=pl.ANY)
    return pl.pallas_call(
        functools.partial(chip_kernel, G, B, N),
        out_shape=jax.ShapeDtypeStruct((R, out_weight.shape[1]), bf),
        in_specs=[anywhere] * 4,
        out_specs=pl.BlockSpec(memory_space=pltpu.VMEM),
        scratch_shapes=[
            pltpu.VMEM((R, features), bf),
            pltpu.VMEM((R, features), bf),
            pltpu.VMEM((R, features), bf),
            pltpu.VMEM((H, R2, WIDE), bf),
            pltpu.VMEM((H, R, WIDE), bf),
            pltpu.VMEM((2, G, 2, C, R, WIDE), bf),
            pltpu.VMEM((G + 1, C, R2, WIDE), bf),
            pltpu.VMEM((G + 1, C, R, WIDE), bf),
            pltpu.VMEM((2, C // 2 * R, B // G * R), f32),
            pltpu.VMEM((2, C // 2 * R, B // G * R), bf),
            pltpu.VMEM((2, C // 2 * R, WIDE), f32),
            pltpu.VMEM((G + 1, C * R, WIDE), f32),
            pltpu.VMEM((G + 1, C * R, WIDE), f32),
            pltpu.VMEM((G + 1, C, R2, WIDE), bf),
            pltpu.VMEM((H, R2, WIDE), bf),
            pltpu.VMEM((R, features), bf),
            pltpu.VMEM(out_weight.shape, bf),
            dma((3,)),
            dma((2,)), dma((2, G, C)),
            dma((2,)), dma((G + 1, C)),
            dma(()),
            dma((2,)), dma((2, G)),
            dma((G + 1,)), dma((H,)),
            dma(()),
        ],
        compiler_params=pltpu.CompilerParams(
            collective_id=0, has_side_effects=True, vmem_limit_bytes=60 * 1024 * 1024
        ),
        name="attention",
    )(query, key, value, out_weight)


def per_device(query, key, value, out_weight):
    R, features = query.shape
    H = features // HD
    R2 = R // 2
    nblk, N = lax.axis_size("blk"), lax.axis_size("node")
    B = nblk * N
    G = groups_of(nblk, H)
    hg = H // G
    NS = (H + B - 2) // B + 1
    dma = pltpu.SemaphoreType.DMA
    bf, f32 = jnp.bfloat16, jnp.float32
    vmem = pl.BlockSpec(memory_space=pltpu.VMEM)
    if G == N and nblk == 2 * G and hg == G + 1 and R % 16 == 0:
        mixed = chip_call(query, key, value, out_weight, G, B, N)
        return lax.psum_scatter(mixed, "pair", scatter_dimension=0, tiled=True)
    mixed = pl.pallas_call(
        functools.partial(kernel, G, B, N),
        out_shape=jax.ShapeDtypeStruct((R, out_weight.shape[1]), bf),
        in_specs=[vmem, vmem, vmem, pl.BlockSpec(memory_space=pl.ANY)],
        out_specs=vmem,
        scratch_shapes=[
            pltpu.VMEM((H, R2, WIDE), bf),
            pltpu.VMEM((H, R, WIDE), bf),
            pltpu.VMEM((max(G - 1, 1), hg, R, WIDE), bf),
            pltpu.VMEM((H, R2, WIDE), bf),
            pltpu.VMEM((NS, B, R, WIDE), bf),
            pltpu.VMEM((NS, B, R, WIDE), bf),
            pltpu.VMEM((H, R, WIDE), bf),
            pltpu.VMEM((H, R, WIDE), f32),
            pltpu.VMEM((H, R, WIDE), f32),
            pltpu.VMEM((H, R2, WIDE), bf),
            pltpu.VMEM((H, R2, WIDE), bf),
            pltpu.VMEM((R, features), bf),
            pltpu.VMEM(out_weight.shape, bf),
            dma((max(G - 1, 1),)),
            dma((max(G - 1, 1),)),
            dma((H,)),
            dma((H,)),
            dma((G, B // G, NS)),
            dma((NS, B)),
            dma((H,)),
            dma((H,)),
            dma(()),
        ],
        compiler_params=pltpu.CompilerParams(
            collective_id=0, has_side_effects=True, vmem_limit_bytes=60 * 1024 * 1024
        ),
        name="attention",
    )(query, key, value, out_weight)
    return lax.psum_scatter(mixed, "pair", scatter_dimension=0, tiled=True)


def solution(mesh):
    in_specs = (
        P(("grp", "blk", "node"), "pair"),
        P(("grp", "blk", "node"), "pair"),
        P(("grp", "blk", "node"), "pair"),
        P("pair", None),
    )
    out_specs = P(("grp", "blk", "node", "pair"), None)
    return jax.shard_map(
        per_device, mesh=mesh, in_specs=in_specs, out_specs=out_specs, check_vma=False
    )
```

```python
import functools
import math

import jax
import jax.numpy as jnp
from jax import lax
from jax.experimental import pallas as pl
from jax.experimental.pallas import tpu as pltpu
from jax.sharding import PartitionSpec as P

HD = 64
WIDE = 2 * HD


def groups_of(blk, heads):
    return max(g for g in range(1, blk + 1) if blk % g == 0 and heads % g == 0)


def kernel(
    G, B, N,
    query_ref, key_ref, value_ref, weight_ref, mixed_ref,
    qp, kvp, kvz, qbuf, kvbuf, vbuf, qfull, peaks, accum, opack, oin, attn, weight,
    z_send, z_recv, q_send, q_recv, kv_send, kv_recv, o_send, o_recv, w_sem,
):
    H, R2, _ = qp.shape
    R = kvp.shape[1]
    hg = H // G
    PL = B // G
    inner = PL // N
    NS = kvbuf.shape[0]
    C = math.gcd(H, B)
    blk, node = lax.axis_index("blk"), lax.axis_index("node")
    z = blk // inner
    p = (blk % inner) * N + node
    bf, f32 = jnp.bfloat16, jnp.float32

    load_weight = pltpu.make_async_copy(weight_ref, weight, w_sem)
    load_weight.start()
    barrier = pltpu.get_barrier_semaphore()
    here = blk * N + node

    def greet(d, _):
        other = lax.rem(here + d, B)
        pl.semaphore_signal(
            barrier, inc=1, device_id={"blk": other // N, "node": lax.rem(other, N)},
            device_id_type=pl.DeviceIdType.MESH,
        )
        return 0

    lax.fori_loop(1, B, greet, 0)

    def peer(zz, pp):
        return {"blk": zz * inner + pp // N, "node": pp % N}

    def remote(src, dst, send, recv, zz, pp):
        return pltpu.make_async_remote_copy(
            src_ref=src, dst_ref=dst, send_sem=send, recv_sem=recv,
            device_id=peer(zz, pp), device_id_type=pl.DeviceIdType.MESH,
        )

    half = lax.broadcasted_iota(jnp.int32, (R2, WIDE), 1) < HD
    wide_half = lax.broadcasted_iota(jnp.int32, (R, WIDE), 1) < HD

    for pair in range(H // 2):
        columns = slice(pair * WIDE, (pair + 1) * WIDE)
        block = query_ref[:, columns].astype(f32)
        turned = pltpu.roll(block, HD, 1)
        qp[2 * pair] = jnp.where(half, block[:R2], turned[R2:]).astype(bf)
        qp[2 * pair + 1] = jnp.where(half, turned[:R2], block[R2:]).astype(bf)
    for pair in range(H // 2):
        columns = slice(pair * WIDE, (pair + 1) * WIDE)
        keys = key_ref[:, columns].astype(f32)
        values = value_ref[:, columns].astype(f32)
        kvp[2 * pair] = jnp.where(wide_half, keys, pltpu.roll(values, HD, 1)).astype(bf)
        kvp[2 * pair + 1] = jnp.where(wide_half, pltpu.roll(keys, HD, 1), values).astype(bf)

    pl.semaphore_wait(barrier, B - 1)

    def send_q(i, act):
        row = lax.rem((z + 1) * hg + i, H)
        zz = row // hg
        n = (row - zz * hg) * B + here
        pp = n // H
        u = n - pp * H
        mine = jnp.logical_and(zz == z, pp == p)

        @pl.when(jnp.logical_not(mine))
        def _():
            act(remote(qp.at[row], qbuf.at[u], q_send.at[row], q_recv.at[u], zz, pp))

        return mine, row, u

    def start_q(i, _):
        mine, row, u = send_q(i, lambda c: c.start())

        @pl.when(mine)
        def _():
            pltpu.make_async_copy(qp.at[row], qbuf.at[u], q_recv.at[u]).start()

        return 0

    lax.fori_loop(0, H, start_q, 0)

    def phase1(dz):
        g = lax.rem(z + dz, G)
        return remote(
            kvp.at[pl.ds(g * hg, hg)], kvz.at[dz - 1], z_send.at[dz - 1], z_recv.at[dz - 1], g, p
        )

    for dz in range(1, G):
        phase1(dz).start()

    def first(pp):
        return (pp * H) // B

    def last(pp):
        return (pp * H + H - 1) // B

    def kv_src(s, h):
        return kvp.at[z * hg + h] if s == 0 else kvz.at[s - 1, h]

    def share_kv(s, act):
        b = s * PL + p

        def one(dp, _):
            pp = lax.rem(p + dp, PL)
            for slot in range(NS):
                @pl.when(first(pp) + slot <= last(pp))
                def _():
                    act(remote(
                        kv_src(s, first(pp) + slot), kvbuf.at[slot, b],
                        kv_send.at[s, dp, slot], kv_recv.at[slot, b], z, pp,
                    ))
            return 0

        lax.fori_loop(1, PL, one, 0)

    def own_kv(s):
        b = s * PL + p
        for slot in range(NS):
            @pl.when(first(p) + slot <= last(p))
            def _():
                pltpu.make_async_copy(kv_src(s, first(p) + slot), kvbuf.at[slot, b], kv_recv.at[slot, b]).start()

    start = lambda c: c.start()
    share_kv(0, start)
    own_kv(0)

    scale = 1.0 / math.sqrt(HD)

    def take_q(u, _):
        pltpu.make_async_copy(qbuf.at[u], qbuf.at[u], q_recv.at[u]).wait()
        both = qbuf[u].astype(f32) * scale
        zero = jnp.zeros_like(both)
        qfull[u] = jnp.concatenate(
            [jnp.where(half, both, zero), jnp.where(half, pltpu.roll(both, HD, 1), zero)], axis=0
        ).astype(bf)
        return 0

    def take_kv(low, high):
        for slot in range(NS):
            @pl.when(first(p) + slot <= last(p))
            def _():
                def one(b, _):
                    pltpu.make_async_copy(kvbuf.at[slot, b], kvbuf.at[slot, b], kv_recv.at[slot, b]).wait()
                    vbuf[slot, b] = jnp.where(wide_half, jnp.ones((), bf), kvbuf[slot, b])
                    return 0
                lax.fori_loop(low * PL, high * PL, one, 0)

    def give(u, act):
        n = p * H + u
        h = n // B
        b = n - h * B
        zz, pp = b // PL, lax.rem(b, PL)
        mine = jnp.logical_and(zz == z, pp == p)
        row = z * hg + h

        @pl.when(jnp.logical_not(mine))
        def _():
            act(remote(opack.at[u], oin.at[row], o_send.at[u], o_recv.at[row], zz, pp))

        return mine, row

    def attend(low, high, t):
        slot = (p * H + t * C) // B - first(p)
        keys = kvbuf[slot, low * PL:high * PL].reshape((high - low) * PL * R, WIDE)
        values = vbuf[slot, low * PL:high * PL].reshape((high - low) * PL * R, WIDE)

        def product(c):
            return lax.dot_general(
                qfull[t * C + c], keys, (((1,), (1,)), ((), ())), preferred_element_type=f32
            )

        def soften(c, scores):
            u = t * C + c
            peak = jnp.max(scores, axis=1, keepdims=True)
            if low > 0:
                before = peaks[u]
                peak = jnp.maximum(before[:, :1], peak)
            expo = jnp.exp(scores - peak).astype(bf)
            total = jnp.dot(expo, values, preferred_element_type=f32)
            if low > 0:
                total = total + accum[u] * jnp.exp(before - peak)
            if high < G:
                peaks[u] = jnp.broadcast_to(peak, (R, WIDE))
                accum[u] = total
                return
            turned = pltpu.roll(total, HD, 1)
            opack[u] = jnp.where(
                half, turned[:R2] / total[:R2], total[R2:] / turned[R2:]
            ).astype(bf)

        scores = product(0)
        for c in range(C):
            ahead = product(c + 1) if c + 1 < C else None
            soften(c, scores)
            scores = ahead
        if high < G:
            return
        for i in range(C):
            u = t * C + i
            mine, row = give(u, start)

            @pl.when(mine)
            def _():
                pltpu.make_async_copy(opack.at[u], oin.at[row], o_recv.at[row]).start()

    def relay(s):
        if s < G:
            phase1(s).wait_recv()
            share_kv(s, start)
            own_kv(s)

    stages = [(s, s + 1) for s in range(min(G, 2))]
    stages += [(s, min(s + 2, G)) for s in range(2, G, 2)]
    turns = H // C
    relay(1)
    lax.fori_loop(0, H, take_q, 0)
    for low, high in stages:
        take_kv(low, high)

        def turn(t, _):
            attend(low, high, t)
            return 0

        if high == 2 and low == 1 and G > 3:
            lax.fori_loop(0, turns // 2, turn, 0)
            relay(3)
            lax.fori_loop(turns // 2, turns, turn, 0)
        else:
            lax.fori_loop(0, turns, turn, 0)
        if high == 1:
            relay(2)
        if high >= 2:
            for s in range(high + 2, min(high + 4, G)):
                relay(s)

    for dz in range(1, G):
        phase1(dz).wait_send()
    for s in range(G):
        share_kv(s, lambda c: c.wait_send())

    def end_q(i, _):
        send_q(i, lambda c: c.wait_send())
        return 0

    lax.fori_loop(0, H, end_q, 0)

    def end(u, _):
        give(u, lambda c: c.wait_send())
        pltpu.make_async_copy(oin.at[u], oin.at[u], o_recv.at[u]).wait()
        return 0

    load_weight.wait()
    lax.fori_loop(0, H, end, 0)
    for pair in range(H // 2):
        even, odd = oin[2 * pair].astype(f32), oin[2 * pair + 1].astype(f32)
        attn[:, pair * WIDE:(pair + 1) * WIDE] = jnp.concatenate(
            [
                jnp.where(half, even, pltpu.roll(odd, HD, 1)),
                jnp.where(half, pltpu.roll(even, HD, 1), odd),
            ],
            axis=0,
        ).astype(bf)
    mixed_ref[...] = jnp.dot(attn[...], weight[...], preferred_element_type=f32).astype(bf)


def chip_kernel(
    G, B, N,
    query_ref, key_ref, value_ref, weight_ref, mixed_ref,
    qin, kin, vin, qp, kvp, kv, qbuf, qfull, scored, expos, shift, peaks, accum, opack, oin, attn, weight,
    in_sem, kv_send, kv_recv, q_send, q_recv, s_send, c_send, c_recv, o_send, o_recv, w_sem,
):
    H, R2, _ = qp.shape
    R = kvp.shape[1]
    hg = H // G
    PL = B // G
    inner = PL // N
    C = PL // 2
    blk, node = lax.axis_index("blk"), lax.axis_index("node")
    z, y = blk // inner, blk % inner
    x, c = node // 2, node % 2
    bf, f32 = jnp.bfloat16, jnp.float32

    def column(r):
        return lax.rem(y + r // 2, 2), lax.rem(x + r % 2, 2)

    def at(dz, r, core=None):
        yy, xx = column(r)
        return {
            "blk": lax.rem(z + dz, G) * inner + yy,
            "node": xx * 2 + (c if core is None else core),
        }

    def main_row(dz, r):
        yy, xx = column(r)
        return lax.rem(z + dz, G) * hg + yy * 2 + xx

    def last_row(dz):
        return lax.rem(z + dz, G) * hg + C

    def remote(src, dst, send, recv, peer):
        return pltpu.make_async_remote_copy(
            src_ref=src, dst_ref=dst, send_sem=send, recv_sem=recv,
            device_id=peer, device_id_type=pl.DeviceIdType.MESH,
        )

    def arrived(ref, sem):
        pltpu.make_async_copy(ref, ref, sem).wait()

    loads = [
        pltpu.make_async_copy(ref, buf, in_sem.at[n])
        for n, (ref, buf) in enumerate(((key_ref, kin), (value_ref, vin), (query_ref, qin)))
    ]
    for load in loads:
        load.start()
    partner = at(0, 0, 1 - c)
    pairs = [(dz, r) for dz in range(G) for r in range(C) if dz or r]
    barrier = pltpu.get_barrier_semaphore()
    for peer in [partner] + [at(dz, r) for dz, r in pairs]:
        pl.semaphore_signal(barrier, inc=1, device_id=peer, device_id_type=pl.DeviceIdType.MESH)
    load_weight = pltpu.make_async_copy(weight_ref, weight, w_sem)
    load_weight.start()

    peaks[...] = jnp.full(peaks.shape, jnp.finfo(f32).min, f32)
    accum[...] = jnp.zeros(accum.shape, f32)
    scored[...] = jnp.full(scored.shape, -jnp.inf, f32)
    expos[...] = jnp.zeros(expos.shape, bf)
    shift[...] = jnp.ones(shift.shape, f32)
    half = lax.broadcasted_iota(jnp.int32, (R2, WIDE), 1) < HD
    wide_half = lax.broadcasted_iota(jnp.int32, (R, WIDE), 1) < HD

    loads[0].wait()
    loads[1].wait()
    for pair in range(H // 2):
        columns = slice(pair * WIDE, (pair + 1) * WIDE)
        keys = kin[:, columns].astype(f32)
        values = vin[:, columns].astype(f32)
        kvp[2 * pair] = jnp.where(wide_half, keys, pltpu.roll(values, HD, 1)).astype(bf)
        kvp[2 * pair + 1] = jnp.where(wide_half, pltpu.roll(keys, HD, 1), values).astype(bf)
    loads[2].wait()
    for pair in range(H // 2):
        columns = slice(pair * WIDE, (pair + 1) * WIDE)
        block = qin[:, columns].astype(f32)
        turned = pltpu.roll(block, HD, 1)
        qp[2 * pair] = jnp.where(half, block[:R2], turned[R2:]).astype(bf)
        qp[2 * pair + 1] = jnp.where(half, turned[:R2], block[R2:]).astype(bf)
    kv[0, 0, 0, 0] = kvp[main_row(0, 0)]
    kv[1, 0, 0, 0] = kvp[last_row(0)]
    qbuf[0, 0] = qp[main_row(0, 0)]
    qbuf[G, 0] = qp[last_row(0)]

    pl.semaphore_wait(barrier, len(pairs) + 1)

    def send_kv(dz, r):
        return remote(kvp.at[main_row(dz, r)], kv.at[0, dz, 0, r], kv_send.at[0], kv_recv.at[0, dz, r], at(dz, r))

    def send_q(dz, r):
        return remote(qp.at[main_row(dz, r)], qbuf.at[dz, r], q_send.at[0], q_recv.at[dz, r], at(dz, r))

    def share(s):
        for r in range(1, C):
            remote(kv.at[1, s, 0, 0], kv.at[1, s, 0, r], s_send, kv_recv.at[1, s, r], at(0, r)).start()

    for r in range(1, C):
        send_kv(0, r).start()
    for r in range(1, C):
        send_q(0, r).start()
    share(0)
    for dz in range(1, G):
        for r in range(C):
            send_q(dz, r).start()
    for dz in range(1, G):
        remote(qp.at[last_row(dz)], qbuf.at[G, dz], q_send.at[1], q_recv.at[G, dz], at(dz, 0)).start()
    def send_near():
        for dz in range(1, G, 2):
            for r in range(C):
                send_kv(dz, r).start()

    def send_shared():
        for dz in range(1, G):
            remote(kvp.at[last_row(dz)], kv.at[1, dz, 0, 0], kv_send.at[1], kv_recv.at[1, dz, 0], at(dz, 0)).start()

    def send_far():
        for dz in range(2, G, 2):
            for r in range(C):
                send_kv(dz, r).start()

    def cross(kind, s):
        for r in range(1 if kind or isinstance(s, int) and s == 0 else 0, C):
            arrived(kv.at[kind, s, 0, r], kv_recv.at[kind, s, r])
        remote(kv.at[kind, s, 0], kv.at[kind, s, 1], c_send.at[kind], c_recv.at[kind, s], partner).start()

    def spread(s):
        arrived(kv.at[1, s, 0, 0], kv_recv.at[1, s, 0])
        share(s)

    scale = 1.0 / math.sqrt(HD)

    def widen(u, b):
        both = qbuf[u, b].astype(f32) * scale
        zero = jnp.zeros_like(both)
        qfull[u, b] = jnp.concatenate(
            [jnp.where(half, both, zero), jnp.where(half, pltpu.roll(both, HD, 1), zero)], axis=0
        ).astype(bf)

    def give(u, b):
        last = u == G
        plane = lax.rem(z + G - jnp.where(last, b, u), G)
        yy, xx = column(b)
        row = jnp.where(last, last_row(0), main_row(0, 0))
        return remote(
            opack.at[u, b], oin.at[row], o_send.at[u], o_recv.at[row],
            {
                "blk": plane * inner + jnp.where(last, y, yy),
                "node": jnp.where(last, x, xx) * 2 + c,
            },
        )

    PART = C // 2
    M = PART * R
    first_half = lax.broadcasted_iota(jnp.int32, (PL * R, WIDE), 1) < HD

    planes_order = [0] + list(range(1, G, 2)) + list(range(2, G, 2))
    first = jnp.where(z == G // 2, G - 1, 1)
    order = [0, first, G - first, G] + list(range(2, G, 2))
    MID = 3

    def pick(index, values):
        found = values[-1]
        for n, value in enumerate(values[:-1]):
            found = jnp.where(index == n, value, found)
        return found

    def unit(k, m):
        if k == MID:
            return G, pick(m, planes_order)
        if k == G:
            m = pick(m, list(range(2, G, 2)) + list(range(1, G, 2)) + [0])
        return m, order[k]

    def before(k, m):
        u, s = unit(k, jnp.maximum(m - 1, 0))
        if k == 0:
            return u, s
        v, w = unit(k - 1, jnp.int32(G - 1))
        return jnp.where(m == 0, v, u), jnp.where(m == 0, w, s)

    def keys_of(u, s):
        return kv[u // G, s].reshape(PL * R, WIDE)

    def values_of(u, s):
        return jnp.where(first_half, jnp.ones((), bf), keys_of(u, s))

    def product(part, u, keys):
        return lax.dot_general(
            qfull[u, part * PART:(part + 1) * PART].reshape(M, WIDE), keys,
            (((1,), (1,)), ((), ())), preferred_element_type=f32,
        )

    def soften(part, u):
        rows = slice(part * M, (part + 1) * M)
        scores = scored[part]
        before = peaks[u, rows]
        peak = jnp.maximum(before, jnp.max(scores, axis=1, keepdims=True))
        peaks[u, rows] = peak
        shift[part] = jnp.exp(before - peak)
        expos[part] = jnp.exp(scores - peak[:, :1]).astype(bf)

    def gather(part, u, values):
        rows = slice(part * M, (part + 1) * M)
        total = jnp.dot(expos[part], values, preferred_element_type=f32)
        accum[u, rows] = total + accum[u, rows] * shift[part]

    def divide(u, b):
        total = accum[u, b * R:(b + 1) * R]
        turned = pltpu.roll(total, HD, 1)
        above = jnp.where(half, turned[:R2], total[R2:])
        below = jnp.where(half, total[:R2], turned[R2:])
        opack[u, b] = (above / below).astype(bf)

    def deliver(u, b):
        if b:
            give(u, b).start()
            return
        stays = jnp.logical_or(u == 0, u == G)

        @pl.when(stays)
        def _():
            oin[jnp.where(u == G, last_row(0), main_row(0, 0))] = opack[u, 0]

        @pl.when(jnp.logical_not(stays))
        def _():
            give(u, 0).start()

    inside = jnp.logical_and(z > 0, z < G - 1)

    @pl.when(inside)
    def _():
        send_near()
        send_shared()
        send_far()

    cross(0, 0)

    @pl.when(jnp.logical_not(inside))
    def _():
        send_near()

    stages = {4: send_shared, 8: send_far}
    steps = {
        3: [(cross, 0, first)],
        6: [(cross, 0, G - first), (cross, 1, 0)],
        8: [(spread, 1)],
        9: [(spread, 3)],
        11: [(spread, 2)],
        12: [(cross, 1, 1)],
        13: [(cross, 1, 3)],
        14: [(cross, 1, 2)],
        15: [(cross, 0, 2)],
    }

    def tick(k, m, _, ending=False):
        u, s = unit(k, m)
        v, w = before(k, m)
        for n, stage in stages.items():
            if n // G == k and not ending:
                pl.when(jnp.logical_and(m == n % G, jnp.logical_not(inside)))(stage)
        for n, step in steps.items():
            if n // G == k and not ending:
                @pl.when(m == n % G)
                def _():
                    for act, *where in step:
                        act(*where)

        if not ending:
            kind = int(k == MID)
            pl.when(jnp.logical_or(kind == 1, m == 0))(
                lambda: arrived(kv.at[kind, s, 1], c_recv.at[kind, s])
            )
        if k == 0:
            for b in range(C):
                @pl.when(jnp.logical_or(b > 0, u > 0))
                def _():
                    arrived(qbuf.at[u, b], q_recv.at[u, b])
                widen(u, b)
        elif k == MID:
            @pl.when(m == 0)
            def _():
                for b in range(C):
                    if b:
                        arrived(qbuf.at[u, b], q_recv.at[u, b])
                    widen(u, b)

        keys, values = keys_of(u, s), values_of(v, w)
        scored[0] = product(0, u, keys)
        gather(0, v, values)
        soften(1, v)
        scored[1] = product(1, u, keys)
        soften(0, u)
        gather(1, v, values)
        if ending:
            for b in range(C):
                divide(v, b)
            for b in range(C):
                deliver(v, b)
        elif k == MID + 1:
            for b in range(C):
                divide(v, b)
                deliver(v, b)
        return 0

    for k in range(MID + 1):
        lax.fori_loop(0, G, functools.partial(tick, k), 0)
    tick(MID + 1, jnp.int32(0), 0)
    lax.fori_loop(1, G, functools.partial(tick, MID + 1, ending=True), 0)
    v, w = unit(MID + 1, jnp.int32(G - 1))
    values = values_of(v, w)
    gather(0, v, values)
    soften(1, v)
    for b in range(PART):
        divide(v, b)
        deliver(v, b)
    gather(1, v, values)
    for b in range(PART, C):
        divide(v, b)
        deliver(v, b)

    load_weight.wait()
    for dz in range(1, G):
        arrived(oin.at[last_row(dz)], o_recv.at[last_row(dz)])
    for dz, r in pairs:
        arrived(oin.at[main_row(dz, r)], o_recv.at[main_row(dz, r)])
    for pair in range(H // 2):
        even, odd = oin[2 * pair].astype(f32), oin[2 * pair + 1].astype(f32)
        attn[:, pair * WIDE:(pair + 1) * WIDE] = jnp.concatenate(
            [
                jnp.where(half, even, pltpu.roll(odd, HD, 1)),
                jnp.where(half, pltpu.roll(even, HD, 1), odd),
            ],
            axis=0,
        ).astype(bf)
    mixed_ref[...] = jnp.dot(attn[...], weight[...], preferred_element_type=f32).astype(bf)

    arrived(kvp.at[0:len(pairs)], kv_send.at[0])
    arrived(kvp.at[0:G - 1], kv_send.at[1])
    arrived(qp.at[0:len(pairs)], q_send.at[0])
    arrived(qp.at[0:G - 1], q_send.at[1])
    arrived(kvp.at[0:G * (C - 1)], s_send)
    for kind in range(2):
        arrived(kvp.at[0:G * C], c_send.at[kind])
    for u in range(G + 1):
        arrived(qp.at[0:C - (1 if u in (0, G) else 0)], o_send.at[u])


def chip_call(query, key, value, out_weight, G, B, N):
    R, features = query.shape
    H = features // HD
    R2 = R // 2
    C = B // G // 2
    dma = pltpu.SemaphoreType.DMA
    bf, f32 = jnp.bfloat16, jnp.float32
    anywhere = pl.BlockSpec(memory_space=pl.ANY)
    return pl.pallas_call(
        functools.partial(chip_kernel, G, B, N),
        out_shape=jax.ShapeDtypeStruct((R, out_weight.shape[1]), bf),
        in_specs=[anywhere] * 4,
        out_specs=pl.BlockSpec(memory_space=pltpu.VMEM),
        scratch_shapes=[
            pltpu.VMEM((R, features), bf),
            pltpu.VMEM((R, features), bf),
            pltpu.VMEM((R, features), bf),
            pltpu.VMEM((H, R2, WIDE), bf),
            pltpu.VMEM((H, R, WIDE), bf),
            pltpu.VMEM((2, G, 2, C, R, WIDE), bf),
            pltpu.VMEM((G + 1, C, R2, WIDE), bf),
            pltpu.VMEM((G + 1, C, R, WIDE), bf),
            pltpu.VMEM((2, C // 2 * R, B // G * R), f32),
            pltpu.VMEM((2, C // 2 * R, B // G * R), bf),
            pltpu.VMEM((2, C // 2 * R, WIDE), f32),
            pltpu.VMEM((G + 1, C * R, WIDE), f32),
            pltpu.VMEM((G + 1, C * R, WIDE), f32),
            pltpu.VMEM((G + 1, C, R2, WIDE), bf),
            pltpu.VMEM((H, R2, WIDE), bf),
            pltpu.VMEM((R, features), bf),
            pltpu.VMEM(out_weight.shape, bf),
            dma((3,)),
            dma((2,)), dma((2, G, C)),
            dma((2,)), dma((G + 1, C)),
            dma(()),
            dma((2,)), dma((2, G)),
            dma((G + 1,)), dma((H,)),
            dma(()),
        ],
        compiler_params=pltpu.CompilerParams(
            collective_id=0, has_side_effects=True, vmem_limit_bytes=54656 * 1024
        ),
        name="attention",
    )(query, key, value, out_weight)


def per_device(query, key, value, out_weight):
    R, features = query.shape
    H = features // HD
    R2 = R // 2
    nblk, N = lax.axis_size("blk"), lax.axis_size("node")
    B = nblk * N
    G = groups_of(nblk, H)
    hg = H // G
    NS = (H + B - 2) // B + 1
    dma = pltpu.SemaphoreType.DMA
    bf, f32 = jnp.bfloat16, jnp.float32
    vmem = pl.BlockSpec(memory_space=pltpu.VMEM)
    if G == N and nblk == 2 * G and hg == G + 1 and R % 16 == 0:
        mixed = chip_call(query, key, value, out_weight, G, B, N)
        return lax.psum_scatter(mixed, "pair", scatter_dimension=0, tiled=True)
    mixed = pl.pallas_call(
        functools.partial(kernel, G, B, N),
        out_shape=jax.ShapeDtypeStruct((R, out_weight.shape[1]), bf),
        in_specs=[vmem, vmem, vmem, pl.BlockSpec(memory_space=pl.ANY)],
        out_specs=vmem,
        scratch_shapes=[
            pltpu.VMEM((H, R2, WIDE), bf),
            pltpu.VMEM((H, R, WIDE), bf),
            pltpu.VMEM((max(G - 1, 1), hg, R, WIDE), bf),
            pltpu.VMEM((H, R2, WIDE), bf),
            pltpu.VMEM((NS, B, R, WIDE), bf),
            pltpu.VMEM((NS, B, R, WIDE), bf),
            pltpu.VMEM((H, R, WIDE), bf),
            pltpu.VMEM((H, R, WIDE), f32),
            pltpu.VMEM((H, R, WIDE), f32),
            pltpu.VMEM((H, R2, WIDE), bf),
            pltpu.VMEM((H, R2, WIDE), bf),
            pltpu.VMEM((R, features), bf),
            pltpu.VMEM(out_weight.shape, bf),
            dma((max(G - 1, 1),)),
            dma((max(G - 1, 1),)),
            dma((H,)),
            dma((H,)),
            dma((G, B // G, NS)),
            dma((NS, B)),
            dma((H,)),
            dma((H,)),
            dma(()),
        ],
        compiler_params=pltpu.CompilerParams(
            collective_id=0, has_side_effects=True, vmem_limit_bytes=60 * 1024 * 1024
        ),
        name="attention",
    )(query, key, value, out_weight)
    return lax.psum_scatter(mixed, "pair", scatter_dimension=0, tiled=True)


def solution(mesh):
    in_specs = (
        P(("grp", "blk", "node"), "pair"),
        P(("grp", "blk", "node"), "pair"),
        P(("grp", "blk", "node"), "pair"),
        P("pair", None),
    )
    out_specs = P(("grp", "blk", "node", "pair"), None)
    return jax.shard_map(
        per_device, mesh=mesh, in_specs=in_specs, out_specs=out_specs, check_vma=False
    )
```

```python
import functools
import math

import jax
import jax.numpy as jnp
from jax import lax
from jax.experimental import pallas as pl
from jax.experimental.pallas import tpu as pltpu
from jax.sharding import PartitionSpec as P

HD = 64
WIDE = 2 * HD


def groups_of(blk, heads):
    return max(g for g in range(1, blk + 1) if blk % g == 0 and heads % g == 0)


def kernel(
    G, B, N,
    query_ref, key_ref, value_ref, weight_ref, mixed_ref,
    qp, kvp, kvz, qbuf, kvbuf, vbuf, qfull, peaks, accum, opack, oin, attn, weight,
    z_send, z_recv, q_send, q_recv, kv_send, kv_recv, o_send, o_recv, w_sem,
):
    H, R2, _ = qp.shape
    R = kvp.shape[1]
    hg = H // G
    PL = B // G
    inner = PL // N
    NS = kvbuf.shape[0]
    C = math.gcd(H, B)
    blk, node = lax.axis_index("blk"), lax.axis_index("node")
    z = blk // inner
    p = (blk % inner) * N + node
    bf, f32 = jnp.bfloat16, jnp.float32

    load_weight = pltpu.make_async_copy(weight_ref, weight, w_sem)
    load_weight.start()
    barrier = pltpu.get_barrier_semaphore()
    here = blk * N + node

    def greet(d, _):
        other = lax.rem(here + d, B)
        pl.semaphore_signal(
            barrier, inc=1, device_id={"blk": other // N, "node": lax.rem(other, N)},
            device_id_type=pl.DeviceIdType.MESH,
        )
        return 0

    lax.fori_loop(1, B, greet, 0)

    def peer(zz, pp):
        return {"blk": zz * inner + pp // N, "node": pp % N}

    def remote(src, dst, send, recv, zz, pp):
        return pltpu.make_async_remote_copy(
            src_ref=src, dst_ref=dst, send_sem=send, recv_sem=recv,
            device_id=peer(zz, pp), device_id_type=pl.DeviceIdType.MESH,
        )

    half = lax.broadcasted_iota(jnp.int32, (R2, WIDE), 1) < HD
    wide_half = lax.broadcasted_iota(jnp.int32, (R, WIDE), 1) < HD

    for pair in range(H // 2):
        columns = slice(pair * WIDE, (pair + 1) * WIDE)
        block = query_ref[:, columns].astype(f32)
        turned = pltpu.roll(block, HD, 1)
        qp[2 * pair] = jnp.where(half, block[:R2], turned[R2:]).astype(bf)
        qp[2 * pair + 1] = jnp.where(half, turned[:R2], block[R2:]).astype(bf)
    for pair in range(H // 2):
        columns = slice(pair * WIDE, (pair + 1) * WIDE)
        keys = key_ref[:, columns].astype(f32)
        values = value_ref[:, columns].astype(f32)
        kvp[2 * pair] = jnp.where(wide_half, keys, pltpu.roll(values, HD, 1)).astype(bf)
        kvp[2 * pair + 1] = jnp.where(wide_half, pltpu.roll(keys, HD, 1), values).astype(bf)

    pl.semaphore_wait(barrier, B - 1)

    def send_q(i, act):
        row = lax.rem((z + 1) * hg + i, H)
        zz = row // hg
        n = (row - zz * hg) * B + here
        pp = n // H
        u = n - pp * H
        mine = jnp.logical_and(zz == z, pp == p)

        @pl.when(jnp.logical_not(mine))
        def _():
            act(remote(qp.at[row], qbuf.at[u], q_send.at[row], q_recv.at[u], zz, pp))

        return mine, row, u

    def start_q(i, _):
        mine, row, u = send_q(i, lambda c: c.start())

        @pl.when(mine)
        def _():
            pltpu.make_async_copy(qp.at[row], qbuf.at[u], q_recv.at[u]).start()

        return 0

    lax.fori_loop(0, H, start_q, 0)

    def phase1(dz):
        g = lax.rem(z + dz, G)
        return remote(
            kvp.at[pl.ds(g * hg, hg)], kvz.at[dz - 1], z_send.at[dz - 1], z_recv.at[dz - 1], g, p
        )

    for dz in range(1, G):
        phase1(dz).start()

    def first(pp):
        return (pp * H) // B

    def last(pp):
        return (pp * H + H - 1) // B

    def kv_src(s, h):
        return kvp.at[z * hg + h] if s == 0 else kvz.at[s - 1, h]

    def share_kv(s, act):
        b = s * PL + p

        def one(dp, _):
            pp = lax.rem(p + dp, PL)
            for slot in range(NS):
                @pl.when(first(pp) + slot <= last(pp))
                def _():
                    act(remote(
                        kv_src(s, first(pp) + slot), kvbuf.at[slot, b],
                        kv_send.at[s, dp, slot], kv_recv.at[slot, b], z, pp,
                    ))
            return 0

        lax.fori_loop(1, PL, one, 0)

    def own_kv(s):
        b = s * PL + p
        for slot in range(NS):
            @pl.when(first(p) + slot <= last(p))
            def _():
                pltpu.make_async_copy(kv_src(s, first(p) + slot), kvbuf.at[slot, b], kv_recv.at[slot, b]).start()

    start = lambda c: c.start()
    share_kv(0, start)
    own_kv(0)

    scale = 1.0 / math.sqrt(HD)

    def take_q(u, _):
        pltpu.make_async_copy(qbuf.at[u], qbuf.at[u], q_recv.at[u]).wait()
        both = qbuf[u].astype(f32) * scale
        zero = jnp.zeros_like(both)
        qfull[u] = jnp.concatenate(
            [jnp.where(half, both, zero), jnp.where(half, pltpu.roll(both, HD, 1), zero)], axis=0
        ).astype(bf)
        return 0

    def take_kv(low, high):
        for slot in range(NS):
            @pl.when(first(p) + slot <= last(p))
            def _():
                def one(b, _):
                    pltpu.make_async_copy(kvbuf.at[slot, b], kvbuf.at[slot, b], kv_recv.at[slot, b]).wait()
                    vbuf[slot, b] = jnp.where(wide_half, jnp.ones((), bf), kvbuf[slot, b])
                    return 0
                lax.fori_loop(low * PL, high * PL, one, 0)

    def give(u, act):
        n = p * H + u
        h = n // B
        b = n - h * B
        zz, pp = b // PL, lax.rem(b, PL)
        mine = jnp.logical_and(zz == z, pp == p)
        row = z * hg + h

        @pl.when(jnp.logical_not(mine))
        def _():
            act(remote(opack.at[u], oin.at[row], o_send.at[u], o_recv.at[row], zz, pp))

        return mine, row

    def attend(low, high, t):
        slot = (p * H + t * C) // B - first(p)
        keys = kvbuf[slot, low * PL:high * PL].reshape((high - low) * PL * R, WIDE)
        values = vbuf[slot, low * PL:high * PL].reshape((high - low) * PL * R, WIDE)

        def product(c):
            return lax.dot_general(
                qfull[t * C + c], keys, (((1,), (1,)), ((), ())), preferred_element_type=f32
            )

        def soften(c, scores):
            u = t * C + c
            peak = jnp.max(scores, axis=1, keepdims=True)
            if low > 0:
                before = peaks[u]
                peak = jnp.maximum(before[:, :1], peak)
            expo = jnp.exp(scores - peak).astype(bf)
            total = jnp.dot(expo, values, preferred_element_type=f32)
            if low > 0:
                total = total + accum[u] * jnp.exp(before - peak)
            if high < G:
                peaks[u] = jnp.broadcast_to(peak, (R, WIDE))
                accum[u] = total
                return
            turned = pltpu.roll(total, HD, 1)
            opack[u] = jnp.where(
                half, turned[:R2] / total[:R2], total[R2:] / turned[R2:]
            ).astype(bf)

        scores = product(0)
        for c in range(C):
            ahead = product(c + 1) if c + 1 < C else None
            soften(c, scores)
            scores = ahead
        if high < G:
            return
        for i in range(C):
            u = t * C + i
            mine, row = give(u, start)

            @pl.when(mine)
            def _():
                pltpu.make_async_copy(opack.at[u], oin.at[row], o_recv.at[row]).start()

    def relay(s):
        if s < G:
            phase1(s).wait_recv()
            share_kv(s, start)
            own_kv(s)

    stages = [(s, s + 1) for s in range(min(G, 2))]
    stages += [(s, min(s + 2, G)) for s in range(2, G, 2)]
    turns = H // C
    relay(1)
    lax.fori_loop(0, H, take_q, 0)
    for low, high in stages:
        take_kv(low, high)

        def turn(t, _):
            attend(low, high, t)
            return 0

        if high == 2 and low == 1 and G > 3:
            lax.fori_loop(0, turns // 2, turn, 0)
            relay(3)
            lax.fori_loop(turns // 2, turns, turn, 0)
        else:
            lax.fori_loop(0, turns, turn, 0)
        if high == 1:
            relay(2)
        if high >= 2:
            for s in range(high + 2, min(high + 4, G)):
                relay(s)

    for dz in range(1, G):
        phase1(dz).wait_send()
    for s in range(G):
        share_kv(s, lambda c: c.wait_send())

    def end_q(i, _):
        send_q(i, lambda c: c.wait_send())
        return 0

    lax.fori_loop(0, H, end_q, 0)

    def end(u, _):
        give(u, lambda c: c.wait_send())
        pltpu.make_async_copy(oin.at[u], oin.at[u], o_recv.at[u]).wait()
        return 0

    load_weight.wait()
    lax.fori_loop(0, H, end, 0)
    for pair in range(H // 2):
        even, odd = oin[2 * pair].astype(f32), oin[2 * pair + 1].astype(f32)
        attn[:, pair * WIDE:(pair + 1) * WIDE] = jnp.concatenate(
            [
                jnp.where(half, even, pltpu.roll(odd, HD, 1)),
                jnp.where(half, pltpu.roll(even, HD, 1), odd),
            ],
            axis=0,
        ).astype(bf)
    mixed_ref[...] = jnp.dot(attn[...], weight[...], preferred_element_type=f32).astype(bf)


def chip_kernel(
    G, B, N,
    query_ref, key_ref, value_ref, weight_ref, mixed_ref,
    qin, kin, vin, qp, kvp, kv, qbuf, qfull, scored, expos, shift, peaks, accum, opack, oin, attn, weight,
    in_sem, kv_send, kv_recv, q_send, q_recv, s_send, c_send, c_recv, o_send, o_recv, w_sem,
):
    H, R2, _ = qp.shape
    R = kvp.shape[1]
    hg = H // G
    PL = B // G
    inner = PL // N
    C = PL // 2
    blk, node = lax.axis_index("blk"), lax.axis_index("node")
    z, y = blk // inner, blk % inner
    x, c = node // 2, node % 2
    bf, f32 = jnp.bfloat16, jnp.float32

    def column(r):
        return lax.rem(y + r // 2, 2), lax.rem(x + r % 2, 2)

    def at(dz, r, core=None):
        yy, xx = column(r)
        return {
            "blk": lax.rem(z + dz, G) * inner + yy,
            "node": xx * 2 + (c if core is None else core),
        }

    def main_row(dz, r):
        yy, xx = column(r)
        return lax.rem(z + dz, G) * hg + yy * 2 + xx

    def last_row(dz):
        return lax.rem(z + dz, G) * hg + C

    def remote(src, dst, send, recv, peer):
        return pltpu.make_async_remote_copy(
            src_ref=src, dst_ref=dst, send_sem=send, recv_sem=recv,
            device_id=peer, device_id_type=pl.DeviceIdType.MESH,
        )

    def arrived(ref, sem):
        pltpu.make_async_copy(ref, ref, sem).wait()

    loads = [
        pltpu.make_async_copy(ref, buf, in_sem.at[n])
        for n, (ref, buf) in enumerate(((key_ref, kin), (value_ref, vin), (query_ref, qin)))
    ]
    for load in loads:
        load.start()
    partner = at(0, 0, 1 - c)
    pairs = [(dz, r) for dz in range(G) for r in range(C) if dz or r]
    barrier = pltpu.get_barrier_semaphore()
    for peer in [partner] + [at(dz, r) for dz, r in pairs]:
        pl.semaphore_signal(barrier, inc=1, device_id=peer, device_id_type=pl.DeviceIdType.MESH)
    load_weight = pltpu.make_async_copy(weight_ref, weight, w_sem)
    load_weight.start()

    peaks[...] = jnp.full(peaks.shape, jnp.finfo(f32).min, f32)
    accum[...] = jnp.zeros(accum.shape, f32)
    scored[...] = jnp.full(scored.shape, -jnp.inf, f32)
    expos[...] = jnp.zeros(expos.shape, bf)
    shift[...] = jnp.ones(shift.shape, f32)
    half = lax.broadcasted_iota(jnp.int32, (R2, WIDE), 1) < HD
    wide_half = lax.broadcasted_iota(jnp.int32, (R, WIDE), 1) < HD

    loads[0].wait()
    loads[1].wait()
    for pair in range(H // 2):
        columns = slice(pair * WIDE, (pair + 1) * WIDE)
        keys = kin[:, columns].astype(f32)
        values = vin[:, columns].astype(f32)
        kvp[2 * pair] = jnp.where(wide_half, keys, pltpu.roll(values, HD, 1)).astype(bf)
        kvp[2 * pair + 1] = jnp.where(wide_half, pltpu.roll(keys, HD, 1), values).astype(bf)
    loads[2].wait()
    for pair in range(H // 2):
        columns = slice(pair * WIDE, (pair + 1) * WIDE)
        block = qin[:, columns].astype(f32)
        turned = pltpu.roll(block, HD, 1)
        qp[2 * pair] = jnp.where(half, block[:R2], turned[R2:]).astype(bf)
        qp[2 * pair + 1] = jnp.where(half, turned[:R2], block[R2:]).astype(bf)
    kv[0, 0, 0, 0] = kvp[main_row(0, 0)]
    kv[1, 0, 0, 0] = kvp[last_row(0)]
    qbuf[0, 0] = qp[main_row(0, 0)]
    qbuf[G, 0] = qp[last_row(0)]

    pl.semaphore_wait(barrier, len(pairs) + 1)

    def send_kv(dz, r):
        return remote(kvp.at[main_row(dz, r)], kv.at[0, dz, 0, r], kv_send.at[0], kv_recv.at[0, dz, r], at(dz, r))

    def send_q(dz, r):
        return remote(qp.at[main_row(dz, r)], qbuf.at[dz, r], q_send.at[0], q_recv.at[dz, r], at(dz, r))

    def share(s):
        for r in range(1, C):
            remote(kv.at[1, s, 0, 0], kv.at[1, s, 0, r], s_send, kv_recv.at[1, s, r], at(0, r)).start()

    for r in range(1, C):
        send_kv(0, r).start()
    for r in range(1, C):
        send_q(0, r).start()
    share(0)
    for dz in range(1, G):
        for r in range(C):
            send_q(dz, r).start()
    for dz in range(1, G):
        remote(qp.at[last_row(dz)], qbuf.at[G, dz], q_send.at[1], q_recv.at[G, dz], at(dz, 0)).start()
    def send_near():
        for dz in range(1, G, 2):
            for r in range(C):
                send_kv(dz, r).start()

    def send_shared():
        for dz in range(1, G):
            remote(kvp.at[last_row(dz)], kv.at[1, dz, 0, 0], kv_send.at[1], kv_recv.at[1, dz, 0], at(dz, 0)).start()

    def send_far():
        for dz in range(2, G, 2):
            for r in range(C):
                send_kv(dz, r).start()

    def cross(kind, s):
        for r in range(1 if kind or isinstance(s, int) and s == 0 else 0, C):
            arrived(kv.at[kind, s, 0, r], kv_recv.at[kind, s, r])
        remote(kv.at[kind, s, 0], kv.at[kind, s, 1], c_send.at[kind], c_recv.at[kind, s], partner).start()

    def spread(s):
        arrived(kv.at[1, s, 0, 0], kv_recv.at[1, s, 0])
        share(s)

    scale = 1.0 / math.sqrt(HD)

    def widen(u, b):
        both = qbuf[u, b].astype(f32) * scale
        zero = jnp.zeros_like(both)
        qfull[u, b] = jnp.concatenate(
            [jnp.where(half, both, zero), jnp.where(half, pltpu.roll(both, HD, 1), zero)], axis=0
        ).astype(bf)

    def give(u, b):
        last = u == G
        plane = lax.rem(z + G - jnp.where(last, b, u), G)
        yy, xx = column(b)
        row = jnp.where(last, last_row(0), main_row(0, 0))
        return remote(
            opack.at[u, b], oin.at[row], o_send.at[u], o_recv.at[row],
            {
                "blk": plane * inner + jnp.where(last, y, yy),
                "node": jnp.where(last, x, xx) * 2 + c,
            },
        )

    PART = C // 2
    M = PART * R
    first_half = lax.broadcasted_iota(jnp.int32, (PL * R, WIDE), 1) < HD

    planes_order = [0] + list(range(1, G, 2)) + list(range(2, G, 2))
    first = jnp.where(z == G // 2, G - 1, 1)
    order = [0, first, G - first, G] + list(range(2, G, 2))
    MID = 3

    def pick(index, values):
        found = values[-1]
        for n, value in enumerate(values[:-1]):
            found = jnp.where(index == n, value, found)
        return found

    def unit(k, m):
        if k == MID:
            return G, pick(m, planes_order)
        if k == G:
            m = pick(m, list(range(2, G, 2)) + list(range(1, G, 2)) + [0])
        return m, order[k]

    def before(k, m):
        u, s = unit(k, jnp.maximum(m - 1, 0))
        if k == 0:
            return u, s
        v, w = unit(k - 1, jnp.int32(G - 1))
        return jnp.where(m == 0, v, u), jnp.where(m == 0, w, s)

    def keys_of(u, s):
        return kv[u // G, s].reshape(PL * R, WIDE)

    def values_of(u, s):
        return jnp.where(first_half, jnp.ones((), bf), keys_of(u, s))

    def product(part, u, keys):
        return lax.dot_general(
            qfull[u, part * PART:(part + 1) * PART].reshape(M, WIDE), keys,
            (((1,), (1,)), ((), ())), preferred_element_type=f32,
        )

    def soften(part, u):
        rows = slice(part * M, (part + 1) * M)
        scores = scored[part]
        before = peaks[u, rows]
        peak = jnp.maximum(before, jnp.max(scores, axis=1, keepdims=True))
        peaks[u, rows] = peak
        shift[part] = jnp.exp(before - peak)
        expos[part] = jnp.exp(scores - peak[:, :1]).astype(bf)

    def gather(part, u, values):
        rows = slice(part * M, (part + 1) * M)
        total = jnp.dot(expos[part], values, preferred_element_type=f32)
        accum[u, rows] = total + accum[u, rows] * shift[part]

    def divide(u, b):
        total = accum[u, b * R:(b + 1) * R]
        turned = pltpu.roll(total, HD, 1)
        above = jnp.where(half, turned[:R2], total[R2:])
        below = jnp.where(half, total[:R2], turned[R2:])
        opack[u, b] = (above / below).astype(bf)

    def deliver(u, b):
        if b:
            give(u, b).start()
            return
        stays = jnp.logical_or(u == 0, u == G)

        @pl.when(stays)
        def _():
            oin[jnp.where(u == G, last_row(0), main_row(0, 0))] = opack[u, 0]

        @pl.when(jnp.logical_not(stays))
        def _():
            give(u, 0).start()

    inside = jnp.logical_and(z > 0, z < G - 1)

    @pl.when(inside)
    def _():
        send_near()
        send_shared()
        send_far()

    cross(0, 0)

    @pl.when(jnp.logical_not(inside))
    def _():
        send_near()

    stages = {4: send_shared, 8: send_far}
    steps = {
        3: [(cross, 0, first)],
        6: [(cross, 0, G - first), (cross, 1, 0)],
        7: [(spread, 1)],
        8: [(spread, 3)],
        9: [(spread, 2)],
        12: [(cross, 1, 1)],
        13: [(cross, 1, 3)],
        14: [(cross, 1, 2)],
        15: [(cross, 0, 2)],
    }

    def tick(k, m, _, ending=False):
        u, s = unit(k, m)
        v, w = before(k, m)
        for n, stage in stages.items():
            if n // G == k and not ending:
                pl.when(jnp.logical_and(m == n % G, jnp.logical_not(inside)))(stage)
        for n, step in steps.items():
            if n // G == k and not ending:
                @pl.when(m == n % G)
                def _():
                    for act, *where in step:
                        act(*where)

        if not ending:
            kind = int(k == MID)
            pl.when(jnp.logical_or(kind == 1, m == 0))(
                lambda: arrived(kv.at[kind, s, 1], c_recv.at[kind, s])
            )
        if k == 0:
            for b in range(C):
                @pl.when(jnp.logical_or(b > 0, u > 0))
                def _():
                    arrived(qbuf.at[u, b], q_recv.at[u, b])
                widen(u, b)
        elif k == MID:
            @pl.when(m == 0)
            def _():
                for b in range(C):
                    if b:
                        arrived(qbuf.at[u, b], q_recv.at[u, b])
                    widen(u, b)

        keys, values = keys_of(u, s), values_of(v, w)
        scored[0] = product(0, u, keys)
        gather(0, v, values)
        if ending:
            for b in range(PART):
                divide(v, b)
        soften(1, v)
        if ending:
            for b in range(PART):
                give(v, b).start()
        scored[1] = product(1, u, keys)
        soften(0, u)
        gather(1, v, values)
        if ending:
            for b in range(PART, C):
                divide(v, b)
                give(v, b).start()
        elif k == MID + 1:
            for b in range(C):
                divide(v, b)
                deliver(v, b)
        return 0

    for k in range(MID + 1):
        lax.fori_loop(0, G, functools.partial(tick, k), 0)
    tick(MID + 1, jnp.int32(0), 0)
    lax.fori_loop(1, G, functools.partial(tick, MID + 1, ending=True), 0)
    v, w = unit(MID + 1, jnp.int32(G - 1))
    values = values_of(v, w)
    gather(0, v, values)
    soften(1, v)
    for b in range(PART):
        divide(v, b)
        deliver(v, b)
    gather(1, v, values)
    for b in range(PART, C):
        divide(v, b)
        deliver(v, b)

    load_weight.wait()
    for dz in range(1, G):
        arrived(oin.at[last_row(dz)], o_recv.at[last_row(dz)])
    for dz, r in pairs:
        arrived(oin.at[main_row(dz, r)], o_recv.at[main_row(dz, r)])
    for pair in range(H // 2):
        even, odd = oin[2 * pair].astype(f32), oin[2 * pair + 1].astype(f32)
        attn[:, pair * WIDE:(pair + 1) * WIDE] = jnp.concatenate(
            [
                jnp.where(half, even, pltpu.roll(odd, HD, 1)),
                jnp.where(half, pltpu.roll(even, HD, 1), odd),
            ],
            axis=0,
        ).astype(bf)
    mixed_ref[...] = jnp.dot(attn[...], weight[...], preferred_element_type=f32).astype(bf)

    arrived(kvp.at[0:len(pairs)], kv_send.at[0])
    arrived(kvp.at[0:G - 1], kv_send.at[1])
    arrived(qp.at[0:len(pairs)], q_send.at[0])
    arrived(qp.at[0:G - 1], q_send.at[1])
    arrived(kvp.at[0:G * (C - 1)], s_send)
    for kind in range(2):
        arrived(kvp.at[0:G * C], c_send.at[kind])
    for u in range(G + 1):
        arrived(qp.at[0:C - (1 if u in (0, G) else 0)], o_send.at[u])


def chip_call(query, key, value, out_weight, G, B, N):
    R, features = query.shape
    H = features // HD
    R2 = R // 2
    C = B // G // 2
    dma = pltpu.SemaphoreType.DMA
    bf, f32 = jnp.bfloat16, jnp.float32
    anywhere = pl.BlockSpec(memory_space=pl.ANY)
    return pl.pallas_call(
        functools.partial(chip_kernel, G, B, N),
        out_shape=jax.ShapeDtypeStruct((R, out_weight.shape[1]), bf),
        in_specs=[anywhere] * 4,
        out_specs=pl.BlockSpec(memory_space=pltpu.VMEM),
        scratch_shapes=[
            pltpu.VMEM((R, features), bf),
            pltpu.VMEM((R, features), bf),
            pltpu.VMEM((R, features), bf),
            pltpu.VMEM((H, R2, WIDE), bf),
            pltpu.VMEM((H, R, WIDE), bf),
            pltpu.VMEM((2, G, 2, C, R, WIDE), bf),
            pltpu.VMEM((G + 1, C, R2, WIDE), bf),
            pltpu.VMEM((G + 1, C, R, WIDE), bf),
            pltpu.VMEM((2, C // 2 * R, B // G * R), f32),
            pltpu.VMEM((2, C // 2 * R, B // G * R), bf),
            pltpu.VMEM((2, C // 2 * R, WIDE), f32),
            pltpu.VMEM((G + 1, C * R, WIDE), f32),
            pltpu.VMEM((G + 1, C * R, WIDE), f32),
            pltpu.VMEM((G + 1, C, R2, WIDE), bf),
            pltpu.VMEM((H, R2, WIDE), bf),
            pltpu.VMEM((R, features), bf),
            pltpu.VMEM(out_weight.shape, bf),
            dma((3,)),
            dma((2,)), dma((2, G, C)),
            dma((2,)), dma((G + 1, C)),
            dma(()),
            dma((2,)), dma((2, G)),
            dma((G + 1,)), dma((H,)),
            dma(()),
        ],
        compiler_params=pltpu.CompilerParams(
            collective_id=0, has_side_effects=True, vmem_limit_bytes=54656 * 1024
        ),
        name="attention",
    )(query, key, value, out_weight)


def per_device(query, key, value, out_weight):
    R, features = query.shape
    H = features // HD
    R2 = R // 2
    nblk, N = lax.axis_size("blk"), lax.axis_size("node")
    B = nblk * N
    G = groups_of(nblk, H)
    hg = H // G
    NS = (H + B - 2) // B + 1
    dma = pltpu.SemaphoreType.DMA
    bf, f32 = jnp.bfloat16, jnp.float32
    vmem = pl.BlockSpec(memory_space=pltpu.VMEM)
    if G == N and nblk == 2 * G and hg == G + 1 and R % 16 == 0:
        mixed = chip_call(query, key, value, out_weight, G, B, N)
        return lax.psum_scatter(mixed, "pair", scatter_dimension=0, tiled=True)
    mixed = pl.pallas_call(
        functools.partial(kernel, G, B, N),
        out_shape=jax.ShapeDtypeStruct((R, out_weight.shape[1]), bf),
        in_specs=[vmem, vmem, vmem, pl.BlockSpec(memory_space=pl.ANY)],
        out_specs=vmem,
        scratch_shapes=[
            pltpu.VMEM((H, R2, WIDE), bf),
            pltpu.VMEM((H, R, WIDE), bf),
            pltpu.VMEM((max(G - 1, 1), hg, R, WIDE), bf),
            pltpu.VMEM((H, R2, WIDE), bf),
            pltpu.VMEM((NS, B, R, WIDE), bf),
            pltpu.VMEM((NS, B, R, WIDE), bf),
            pltpu.VMEM((H, R, WIDE), bf),
            pltpu.VMEM((H, R, WIDE), f32),
            pltpu.VMEM((H, R, WIDE), f32),
            pltpu.VMEM((H, R2, WIDE), bf),
            pltpu.VMEM((H, R2, WIDE), bf),
            pltpu.VMEM((R, features), bf),
            pltpu.VMEM(out_weight.shape, bf),
            dma((max(G - 1, 1),)),
            dma((max(G - 1, 1),)),
            dma((H,)),
            dma((H,)),
            dma((G, B // G, NS)),
            dma((NS, B)),
            dma((H,)),
            dma((H,)),
            dma(()),
        ],
        compiler_params=pltpu.CompilerParams(
            collective_id=0, has_side_effects=True, vmem_limit_bytes=60 * 1024 * 1024
        ),
        name="attention",
    )(query, key, value, out_weight)
    return lax.psum_scatter(mixed, "pair", scatter_dimension=0, tiled=True)


def solution(mesh):
    in_specs = (
        P(("grp", "blk", "node"), "pair"),
        P(("grp", "blk", "node"), "pair"),
        P(("grp", "blk", "node"), "pair"),
        P("pair", None),
    )
    out_specs = P(("grp", "blk", "node", "pair"), None)
    return jax.shard_map(
        per_device, mesh=mesh, in_specs=in_specs, out_specs=out_specs, check_vma=False
    )
```

```python
import functools
import math

import jax
import jax.numpy as jnp
from jax import lax
from jax.experimental import pallas as pl
from jax.experimental.pallas import tpu as pltpu
from jax.sharding import PartitionSpec as P

HD = 64
WIDE = 2 * HD


def groups_of(blk, heads):
    return max(g for g in range(1, blk + 1) if blk % g == 0 and heads % g == 0)


def kernel(
    G, B, N,
    query_ref, key_ref, value_ref, weight_ref, mixed_ref,
    qp, kvp, kvz, qbuf, kvbuf, vbuf, qfull, peaks, accum, opack, oin, attn, weight,
    z_send, z_recv, q_send, q_recv, kv_send, kv_recv, o_send, o_recv, w_sem,
):
    H, R2, _ = qp.shape
    R = kvp.shape[1]
    hg = H // G
    PL = B // G
    inner = PL // N
    NS = kvbuf.shape[0]
    C = math.gcd(H, B)
    blk, node = lax.axis_index("blk"), lax.axis_index("node")
    z = blk // inner
    p = (blk % inner) * N + node
    bf, f32 = jnp.bfloat16, jnp.float32

    load_weight = pltpu.make_async_copy(weight_ref, weight, w_sem)
    load_weight.start()
    barrier = pltpu.get_barrier_semaphore()
    here = blk * N + node

    def greet(d, _):
        other = lax.rem(here + d, B)
        pl.semaphore_signal(
            barrier, inc=1, device_id={"blk": other // N, "node": lax.rem(other, N)},
            device_id_type=pl.DeviceIdType.MESH,
        )
        return 0

    lax.fori_loop(1, B, greet, 0)

    def peer(zz, pp):
        return {"blk": zz * inner + pp // N, "node": pp % N}

    def remote(src, dst, send, recv, zz, pp):
        return pltpu.make_async_remote_copy(
            src_ref=src, dst_ref=dst, send_sem=send, recv_sem=recv,
            device_id=peer(zz, pp), device_id_type=pl.DeviceIdType.MESH,
        )

    half = lax.broadcasted_iota(jnp.int32, (R2, WIDE), 1) < HD
    wide_half = lax.broadcasted_iota(jnp.int32, (R, WIDE), 1) < HD

    for pair in range(H // 2):
        columns = slice(pair * WIDE, (pair + 1) * WIDE)
        block = query_ref[:, columns].astype(f32)
        turned = pltpu.roll(block, HD, 1)
        qp[2 * pair] = jnp.where(half, block[:R2], turned[R2:]).astype(bf)
        qp[2 * pair + 1] = jnp.where(half, turned[:R2], block[R2:]).astype(bf)
    for pair in range(H // 2):
        columns = slice(pair * WIDE, (pair + 1) * WIDE)
        keys = key_ref[:, columns].astype(f32)
        values = value_ref[:, columns].astype(f32)
        kvp[2 * pair] = jnp.where(wide_half, keys, pltpu.roll(values, HD, 1)).astype(bf)
        kvp[2 * pair + 1] = jnp.where(wide_half, pltpu.roll(keys, HD, 1), values).astype(bf)

    pl.semaphore_wait(barrier, B - 1)

    def send_q(i, act):
        row = lax.rem((z + 1) * hg + i, H)
        zz = row // hg
        n = (row - zz * hg) * B + here
        pp = n // H
        u = n - pp * H
        mine = jnp.logical_and(zz == z, pp == p)

        @pl.when(jnp.logical_not(mine))
        def _():
            act(remote(qp.at[row], qbuf.at[u], q_send.at[row], q_recv.at[u], zz, pp))

        return mine, row, u

    def start_q(i, _):
        mine, row, u = send_q(i, lambda c: c.start())

        @pl.when(mine)
        def _():
            pltpu.make_async_copy(qp.at[row], qbuf.at[u], q_recv.at[u]).start()

        return 0

    lax.fori_loop(0, H, start_q, 0)

    def phase1(dz):
        g = lax.rem(z + dz, G)
        return remote(
            kvp.at[pl.ds(g * hg, hg)], kvz.at[dz - 1], z_send.at[dz - 1], z_recv.at[dz - 1], g, p
        )

    for dz in range(1, G):
        phase1(dz).start()

    def first(pp):
        return (pp * H) // B

    def last(pp):
        return (pp * H + H - 1) // B

    def kv_src(s, h):
        return kvp.at[z * hg + h] if s == 0 else kvz.at[s - 1, h]

    def share_kv(s, act):
        b = s * PL + p

        def one(dp, _):
            pp = lax.rem(p + dp, PL)
            for slot in range(NS):
                @pl.when(first(pp) + slot <= last(pp))
                def _():
                    act(remote(
                        kv_src(s, first(pp) + slot), kvbuf.at[slot, b],
                        kv_send.at[s, dp, slot], kv_recv.at[slot, b], z, pp,
                    ))
            return 0

        lax.fori_loop(1, PL, one, 0)

    def own_kv(s):
        b = s * PL + p
        for slot in range(NS):
            @pl.when(first(p) + slot <= last(p))
            def _():
                pltpu.make_async_copy(kv_src(s, first(p) + slot), kvbuf.at[slot, b], kv_recv.at[slot, b]).start()

    start = lambda c: c.start()
    share_kv(0, start)
    own_kv(0)

    scale = 1.0 / math.sqrt(HD)

    def take_q(u, _):
        pltpu.make_async_copy(qbuf.at[u], qbuf.at[u], q_recv.at[u]).wait()
        both = qbuf[u].astype(f32) * scale
        zero = jnp.zeros_like(both)
        qfull[u] = jnp.concatenate(
            [jnp.where(half, both, zero), jnp.where(half, pltpu.roll(both, HD, 1), zero)], axis=0
        ).astype(bf)
        return 0

    def take_kv(low, high):
        for slot in range(NS):
            @pl.when(first(p) + slot <= last(p))
            def _():
                def one(b, _):
                    pltpu.make_async_copy(kvbuf.at[slot, b], kvbuf.at[slot, b], kv_recv.at[slot, b]).wait()
                    vbuf[slot, b] = jnp.where(wide_half, jnp.ones((), bf), kvbuf[slot, b])
                    return 0
                lax.fori_loop(low * PL, high * PL, one, 0)

    def give(u, act):
        n = p * H + u
        h = n // B
        b = n - h * B
        zz, pp = b // PL, lax.rem(b, PL)
        mine = jnp.logical_and(zz == z, pp == p)
        row = z * hg + h

        @pl.when(jnp.logical_not(mine))
        def _():
            act(remote(opack.at[u], oin.at[row], o_send.at[u], o_recv.at[row], zz, pp))

        return mine, row

    def attend(low, high, t):
        slot = (p * H + t * C) // B - first(p)
        keys = kvbuf[slot, low * PL:high * PL].reshape((high - low) * PL * R, WIDE)
        values = vbuf[slot, low * PL:high * PL].reshape((high - low) * PL * R, WIDE)

        def product(c):
            return lax.dot_general(
                qfull[t * C + c], keys, (((1,), (1,)), ((), ())), preferred_element_type=f32
            )

        def soften(c, scores):
            u = t * C + c
            peak = jnp.max(scores, axis=1, keepdims=True)
            if low > 0:
                before = peaks[u]
                peak = jnp.maximum(before[:, :1], peak)
            expo = jnp.exp(scores - peak).astype(bf)
            total = jnp.dot(expo, values, preferred_element_type=f32)
            if low > 0:
                total = total + accum[u] * jnp.exp(before - peak)
            if high < G:
                peaks[u] = jnp.broadcast_to(peak, (R, WIDE))
                accum[u] = total
                return
            turned = pltpu.roll(total, HD, 1)
            opack[u] = jnp.where(
                half, turned[:R2] / total[:R2], total[R2:] / turned[R2:]
            ).astype(bf)

        scores = product(0)
        for c in range(C):
            ahead = product(c + 1) if c + 1 < C else None
            soften(c, scores)
            scores = ahead
        if high < G:
            return
        for i in range(C):
            u = t * C + i
            mine, row = give(u, start)

            @pl.when(mine)
            def _():
                pltpu.make_async_copy(opack.at[u], oin.at[row], o_recv.at[row]).start()

    def relay(s):
        if s < G:
            phase1(s).wait_recv()
            share_kv(s, start)
            own_kv(s)

    stages = [(s, s + 1) for s in range(min(G, 2))]
    stages += [(s, min(s + 2, G)) for s in range(2, G, 2)]
    turns = H // C
    relay(1)
    lax.fori_loop(0, H, take_q, 0)
    for low, high in stages:
        take_kv(low, high)

        def turn(t, _):
            attend(low, high, t)
            return 0

        if high == 2 and low == 1 and G > 3:
            lax.fori_loop(0, turns // 2, turn, 0)
            relay(3)
            lax.fori_loop(turns // 2, turns, turn, 0)
        else:
            lax.fori_loop(0, turns, turn, 0)
        if high == 1:
            relay(2)
        if high >= 2:
            for s in range(high + 2, min(high + 4, G)):
                relay(s)

    for dz in range(1, G):
        phase1(dz).wait_send()
    for s in range(G):
        share_kv(s, lambda c: c.wait_send())

    def end_q(i, _):
        send_q(i, lambda c: c.wait_send())
        return 0

    lax.fori_loop(0, H, end_q, 0)

    def end(u, _):
        give(u, lambda c: c.wait_send())
        pltpu.make_async_copy(oin.at[u], oin.at[u], o_recv.at[u]).wait()
        return 0

    load_weight.wait()
    lax.fori_loop(0, H, end, 0)
    for pair in range(H // 2):
        even, odd = oin[2 * pair].astype(f32), oin[2 * pair + 1].astype(f32)
        attn[:, pair * WIDE:(pair + 1) * WIDE] = jnp.concatenate(
            [
                jnp.where(half, even, pltpu.roll(odd, HD, 1)),
                jnp.where(half, pltpu.roll(even, HD, 1), odd),
            ],
            axis=0,
        ).astype(bf)
    mixed_ref[...] = jnp.dot(attn[...], weight[...], preferred_element_type=f32).astype(bf)


def chip_kernel(
    G, B, N,
    query_ref, key_ref, value_ref, weight_ref, mixed_ref,
    qin, kin, vin, qp, kvp, kv, qbuf, qfull, scored, expos, shift, peaks, accum, opack, oin, attn, weight,
    in_sem, kv_send, kv_recv, q_send, q_recv, s_send, c_send, c_recv, o_send, o_recv, w_sem,
):
    H, R2, _ = qp.shape
    R = kvp.shape[1]
    hg = H // G
    PL = B // G
    inner = PL // N
    C = PL // 2
    blk, node = lax.axis_index("blk"), lax.axis_index("node")
    z, y = blk // inner, blk % inner
    x, c = node // 2, node % 2
    bf, f32 = jnp.bfloat16, jnp.float32

    def column(r):
        return lax.rem(y + r // 2, 2), lax.rem(x + r % 2, 2)

    def at(dz, r, core=None):
        yy, xx = column(r)
        return {
            "blk": lax.rem(z + dz, G) * inner + yy,
            "node": xx * 2 + (c if core is None else core),
        }

    def main_row(dz, r):
        yy, xx = column(r)
        return lax.rem(z + dz, G) * hg + yy * 2 + xx

    def last_row(dz):
        return lax.rem(z + dz, G) * hg + C

    def remote(src, dst, send, recv, peer):
        return pltpu.make_async_remote_copy(
            src_ref=src, dst_ref=dst, send_sem=send, recv_sem=recv,
            device_id=peer, device_id_type=pl.DeviceIdType.MESH,
        )

    def arrived(ref, sem):
        pltpu.make_async_copy(ref, ref, sem).wait()

    loads = [
        pltpu.make_async_copy(ref, buf, in_sem.at[n])
        for n, (ref, buf) in enumerate(((key_ref, kin), (value_ref, vin), (query_ref, qin)))
    ]
    for load in loads:
        load.start()
    partner = at(0, 0, 1 - c)
    pairs = [(dz, r) for dz in range(G) for r in range(C) if dz or r]
    barrier = pltpu.get_barrier_semaphore()
    for peer in [partner] + [at(dz, r) for dz, r in pairs]:
        pl.semaphore_signal(barrier, inc=1, device_id=peer, device_id_type=pl.DeviceIdType.MESH)
    load_weight = pltpu.make_async_copy(weight_ref, weight, w_sem)
    load_weight.start()

    peaks[...] = jnp.full(peaks.shape, jnp.finfo(f32).min, f32)
    accum[...] = jnp.zeros(accum.shape, f32)
    scored[...] = jnp.full(scored.shape, -jnp.inf, f32)
    expos[...] = jnp.zeros(expos.shape, bf)
    shift[...] = jnp.ones(shift.shape, f32)
    half = lax.broadcasted_iota(jnp.int32, (R2, WIDE), 1) < HD
    wide_half = lax.broadcasted_iota(jnp.int32, (R, WIDE), 1) < HD

    loads[0].wait()
    loads[1].wait()
    for pair in range(H // 2):
        columns = slice(pair * WIDE, (pair + 1) * WIDE)
        keys = kin[:, columns].astype(f32)
        values = vin[:, columns].astype(f32)
        kvp[2 * pair] = jnp.where(wide_half, keys, pltpu.roll(values, HD, 1)).astype(bf)
        kvp[2 * pair + 1] = jnp.where(wide_half, pltpu.roll(keys, HD, 1), values).astype(bf)
    loads[2].wait()
    for pair in range(H // 2):
        columns = slice(pair * WIDE, (pair + 1) * WIDE)
        block = qin[:, columns].astype(f32)
        turned = pltpu.roll(block, HD, 1)
        qp[2 * pair] = jnp.where(half, block[:R2], turned[R2:]).astype(bf)
        qp[2 * pair + 1] = jnp.where(half, turned[:R2], block[R2:]).astype(bf)
    kv[0, 0, 0, 0] = kvp[main_row(0, 0)]
    kv[1, 0, 0, 0] = kvp[last_row(0)]
    qbuf[0, 0] = qp[main_row(0, 0)]
    qbuf[G, 0] = qp[last_row(0)]

    pl.semaphore_wait(barrier, len(pairs) + 1)

    def send_kv(dz, r):
        return remote(kvp.at[main_row(dz, r)], kv.at[0, dz, 0, r], kv_send.at[0], kv_recv.at[0, dz, r], at(dz, r))

    def send_q(dz, r):
        return remote(qp.at[main_row(dz, r)], qbuf.at[dz, r], q_send.at[0], q_recv.at[dz, r], at(dz, r))

    def share(s):
        for r in range(1, C):
            remote(kv.at[1, s, 0, 0], kv.at[1, s, 0, r], s_send, kv_recv.at[1, s, r], at(0, r)).start()

    for r in range(1, C):
        send_kv(0, r).start()
    for r in range(1, C):
        send_q(0, r).start()
    for dz in range(1, G):
        for r in range(C):
            send_q(dz, r).start()
    for dz in range(1, G):
        remote(qp.at[last_row(dz)], qbuf.at[G, dz], q_send.at[1], q_recv.at[G, dz], at(dz, 0)).start()
    def send_near():
        for dz in range(1, G, 2):
            for r in range(C):
                send_kv(dz, r).start()

    def send_shared():
        for dz in range(1, G):
            remote(kvp.at[last_row(dz)], kv.at[1, dz, 0, 0], kv_send.at[1], kv_recv.at[1, dz, 0], at(dz, 0)).start()

    def send_far():
        for dz in range(2, G, 2):
            for r in range(C):
                send_kv(dz, r).start()

    def cross(kind, s):
        for r in range(1 if kind or isinstance(s, int) and s == 0 else 0, C):
            arrived(kv.at[kind, s, 0, r], kv_recv.at[kind, s, r])
        remote(kv.at[kind, s, 0], kv.at[kind, s, 1], c_send.at[kind], c_recv.at[kind, s], partner).start()

    def spread(s):
        arrived(kv.at[1, s, 0, 0], kv_recv.at[1, s, 0])
        share(s)

    scale = 1.0 / math.sqrt(HD)

    def widen(u, b):
        both = qbuf[u, b].astype(f32) * scale
        zero = jnp.zeros_like(both)
        qfull[u, b] = jnp.concatenate(
            [jnp.where(half, both, zero), jnp.where(half, pltpu.roll(both, HD, 1), zero)], axis=0
        ).astype(bf)

    def give(u, b):
        last = u == G
        plane = lax.rem(z + G - jnp.where(last, b, u), G)
        yy, xx = column(b)
        row = jnp.where(last, last_row(0), main_row(0, 0))
        return remote(
            opack.at[u, b], oin.at[row], o_send.at[u], o_recv.at[row],
            {
                "blk": plane * inner + jnp.where(last, y, yy),
                "node": jnp.where(last, x, xx) * 2 + c,
            },
        )

    PART = C // 2
    M = PART * R
    first_half = lax.broadcasted_iota(jnp.int32, (PL * R, WIDE), 1) < HD

    planes_order = [0] + list(range(1, G, 2)) + list(range(2, G, 2))
    first = jnp.where(z == G // 2, G - 1, 1)
    order = [0, first, G - first, G] + list(range(2, G, 2))
    MID = 3

    def pick(index, values):
        found = values[-1]
        for n, value in enumerate(values[:-1]):
            found = jnp.where(index == n, value, found)
        return found

    def unit(k, m):
        if k == MID:
            return G, pick(m, planes_order)
        if k == G:
            m = pick(m, list(range(2, G, 2)) + list(range(1, G, 2)) + [0])
        return m, order[k]

    def before(k, m):
        u, s = unit(k, jnp.maximum(m - 1, 0))
        if k == 0:
            return u, s
        v, w = unit(k - 1, jnp.int32(G - 1))
        return jnp.where(m == 0, v, u), jnp.where(m == 0, w, s)

    def keys_of(u, s):
        return kv[u // G, s].reshape(PL * R, WIDE)

    def values_of(u, s):
        return jnp.where(first_half, jnp.ones((), bf), keys_of(u, s))

    def product(part, u, keys):
        return lax.dot_general(
            qfull[u, part * PART:(part + 1) * PART].reshape(M, WIDE), keys,
            (((1,), (1,)), ((), ())), preferred_element_type=f32,
        )

    def soften(part, u):
        rows = slice(part * M, (part + 1) * M)
        scores = scored[part]
        before = peaks[u, rows]
        peak = jnp.maximum(before, jnp.max(scores, axis=1, keepdims=True))
        peaks[u, rows] = peak
        shift[part] = jnp.exp(before - peak)
        expos[part] = jnp.exp(scores - peak[:, :1]).astype(bf)

    def gather(part, u, values):
        rows = slice(part * M, (part + 1) * M)
        total = jnp.dot(expos[part], values, preferred_element_type=f32)
        accum[u, rows] = total + accum[u, rows] * shift[part]

    def divide(u, b):
        total = accum[u, b * R:(b + 1) * R]
        turned = pltpu.roll(total, HD, 1)
        above = jnp.where(half, turned[:R2], total[R2:])
        below = jnp.where(half, total[:R2], turned[R2:])
        opack[u, b] = (above / below).astype(bf)

    def deliver(u, b):
        if b:
            give(u, b).start()
            return
        stays = jnp.logical_or(u == 0, u == G)

        @pl.when(stays)
        def _():
            oin[jnp.where(u == G, last_row(0), main_row(0, 0))] = opack[u, 0]

        @pl.when(jnp.logical_not(stays))
        def _():
            give(u, 0).start()

    inside = jnp.logical_and(z > 0, z < G - 1)

    @pl.when(inside)
    def _():
        send_near()
        send_shared()
        send_far()

    cross(0, 0)
    share(0)

    @pl.when(jnp.logical_not(inside))
    def _():
        send_near()

    stages = {4: send_shared, 8: send_far}
    steps = {
        3: [(cross, 0, first)],
        6: [(cross, 0, G - first), (cross, 1, 0)],
        7: [(spread, 1)],
        8: [(spread, 3)],
        9: [(spread, 2)],
        12: [(cross, 1, 1)],
        13: [(cross, 1, 3)],
        14: [(cross, 1, 2)],
        15: [(cross, 0, 2)],
    }

    def tick(k, m, _, ending=False):
        u, s = unit(k, m)
        v, w = before(k, m)
        for n, stage in stages.items():
            if n // G == k and not ending:
                pl.when(jnp.logical_and(m == n % G, jnp.logical_not(inside)))(stage)
        for n, step in steps.items():
            if n // G == k and not ending:
                @pl.when(m == n % G)
                def _():
                    for act, *where in step:
                        act(*where)

        if not ending:
            kind = int(k == MID)
            pl.when(jnp.logical_or(kind == 1, m == 0))(
                lambda: arrived(kv.at[kind, s, 1], c_recv.at[kind, s])
            )
        if k == 0:
            for b in range(C):
                @pl.when(jnp.logical_or(b > 0, u > 0))
                def _():
                    arrived(qbuf.at[u, b], q_recv.at[u, b])
                widen(u, b)
        elif k == MID:
            @pl.when(m == 0)
            def _():
                for b in range(C):
                    if b:
                        arrived(qbuf.at[u, b], q_recv.at[u, b])
                    widen(u, b)

        keys, values = keys_of(u, s), values_of(v, w)
        scored[0] = product(0, u, keys)
        gather(0, v, values)
        if ending:
            for b in range(PART):
                divide(v, b)
        soften(1, v)
        if ending:
            for b in range(PART):
                give(v, b).start()
        scored[1] = product(1, u, keys)
        soften(0, u)
        gather(1, v, values)
        if ending:
            for b in range(PART, C):
                divide(v, b)
                give(v, b).start()
        elif k == MID + 1:
            for b in range(C):
                divide(v, b)
                deliver(v, b)
        return 0

    for k in range(MID + 1):
        lax.fori_loop(0, G, functools.partial(tick, k), 0)
    tick(MID + 1, jnp.int32(0), 0)
    lax.fori_loop(1, G, functools.partial(tick, MID + 1, ending=True), 0)
    v, w = unit(MID + 1, jnp.int32(G - 1))
    values = values_of(v, w)
    gather(0, v, values)
    soften(1, v)
    for b in range(PART):
        divide(v, b)
        deliver(v, b)
    gather(1, v, values)
    for b in range(PART, C):
        divide(v, b)
        deliver(v, b)

    load_weight.wait()
    for dz in range(1, G):
        arrived(oin.at[last_row(dz)], o_recv.at[last_row(dz)])
    for dz, r in pairs:
        arrived(oin.at[main_row(dz, r)], o_recv.at[main_row(dz, r)])
    for pair in range(H // 2):
        even, odd = oin[2 * pair].astype(f32), oin[2 * pair + 1].astype(f32)
        attn[:, pair * WIDE:(pair + 1) * WIDE] = jnp.concatenate(
            [
                jnp.where(half, even, pltpu.roll(odd, HD, 1)),
                jnp.where(half, pltpu.roll(even, HD, 1), odd),
            ],
            axis=0,
        ).astype(bf)
    mixed_ref[...] = jnp.dot(attn[...], weight[...], preferred_element_type=f32).astype(bf)

    arrived(kvp.at[0:len(pairs)], kv_send.at[0])
    arrived(kvp.at[0:G - 1], kv_send.at[1])
    arrived(qp.at[0:len(pairs)], q_send.at[0])
    arrived(qp.at[0:G - 1], q_send.at[1])
    arrived(kvp.at[0:G * (C - 1)], s_send)
    for kind in range(2):
        arrived(kvp.at[0:G * C], c_send.at[kind])
    for u in range(G + 1):
        arrived(qp.at[0:C - (1 if u in (0, G) else 0)], o_send.at[u])


def chip_call(query, key, value, out_weight, G, B, N):
    R, features = query.shape
    H = features // HD
    R2 = R // 2
    C = B // G // 2
    dma = pltpu.SemaphoreType.DMA
    bf, f32 = jnp.bfloat16, jnp.float32
    anywhere = pl.BlockSpec(memory_space=pl.ANY)
    return pl.pallas_call(
        functools.partial(chip_kernel, G, B, N),
        out_shape=jax.ShapeDtypeStruct((R, out_weight.shape[1]), bf),
        in_specs=[anywhere] * 4,
        out_specs=pl.BlockSpec(memory_space=pltpu.VMEM),
        scratch_shapes=[
            pltpu.VMEM((R, features), bf),
            pltpu.VMEM((R, features), bf),
            pltpu.VMEM((R, features), bf),
            pltpu.VMEM((H, R2, WIDE), bf),
            pltpu.VMEM((H, R, WIDE), bf),
            pltpu.VMEM((2, G, 2, C, R, WIDE), bf),
            pltpu.VMEM((G + 1, C, R2, WIDE), bf),
            pltpu.VMEM((G + 1, C, R, WIDE), bf),
            pltpu.VMEM((2, C // 2 * R, B // G * R), f32),
            pltpu.VMEM((2, C // 2 * R, B // G * R), bf),
            pltpu.VMEM((2, C // 2 * R, WIDE), f32),
            pltpu.VMEM((G + 1, C * R, WIDE), f32),
            pltpu.VMEM((G + 1, C * R, WIDE), f32),
            pltpu.VMEM((G + 1, C, R2, WIDE), bf),
            pltpu.VMEM((H, R2, WIDE), bf),
            pltpu.VMEM((R, features), bf),
            pltpu.VMEM(out_weight.shape, bf),
            dma((3,)),
            dma((2,)), dma((2, G, C)),
            dma((2,)), dma((G + 1, C)),
            dma(()),
            dma((2,)), dma((2, G)),
            dma((G + 1,)), dma((H,)),
            dma(()),
        ],
        compiler_params=pltpu.CompilerParams(
            collective_id=0, has_side_effects=True, vmem_limit_bytes=54656 * 1024
        ),
        name="attention",
    )(query, key, value, out_weight)


def per_device(query, key, value, out_weight):
    R, features = query.shape
    H = features // HD
    R2 = R // 2
    nblk, N = lax.axis_size("blk"), lax.axis_size("node")
    B = nblk * N
    G = groups_of(nblk, H)
    hg = H // G
    NS = (H + B - 2) // B + 1
    dma = pltpu.SemaphoreType.DMA
    bf, f32 = jnp.bfloat16, jnp.float32
    vmem = pl.BlockSpec(memory_space=pltpu.VMEM)
    if G == N and nblk == 2 * G and hg == G + 1 and R % 16 == 0:
        mixed = chip_call(query, key, value, out_weight, G, B, N)
        return lax.psum_scatter(mixed, "pair", scatter_dimension=0, tiled=True)
    mixed = pl.pallas_call(
        functools.partial(kernel, G, B, N),
        out_shape=jax.ShapeDtypeStruct((R, out_weight.shape[1]), bf),
        in_specs=[vmem, vmem, vmem, pl.BlockSpec(memory_space=pl.ANY)],
        out_specs=vmem,
        scratch_shapes=[
            pltpu.VMEM((H, R2, WIDE), bf),
            pltpu.VMEM((H, R, WIDE), bf),
            pltpu.VMEM((max(G - 1, 1), hg, R, WIDE), bf),
            pltpu.VMEM((H, R2, WIDE), bf),
            pltpu.VMEM((NS, B, R, WIDE), bf),
            pltpu.VMEM((NS, B, R, WIDE), bf),
            pltpu.VMEM((H, R, WIDE), bf),
            pltpu.VMEM((H, R, WIDE), f32),
            pltpu.VMEM((H, R, WIDE), f32),
            pltpu.VMEM((H, R2, WIDE), bf),
            pltpu.VMEM((H, R2, WIDE), bf),
            pltpu.VMEM((R, features), bf),
            pltpu.VMEM(out_weight.shape, bf),
            dma((max(G - 1, 1),)),
            dma((max(G - 1, 1),)),
            dma((H,)),
            dma((H,)),
            dma((G, B // G, NS)),
            dma((NS, B)),
            dma((H,)),
            dma((H,)),
            dma(()),
        ],
        compiler_params=pltpu.CompilerParams(
            collective_id=0, has_side_effects=True, vmem_limit_bytes=60 * 1024 * 1024
        ),
        name="attention",
    )(query, key, value, out_weight)
    return lax.psum_scatter(mixed, "pair", scatter_dimension=0, tiled=True)


def solution(mesh):
    in_specs = (
        P(("grp", "blk", "node"), "pair"),
        P(("grp", "blk", "node"), "pair"),
        P(("grp", "blk", "node"), "pair"),
        P("pair", None),
    )
    out_specs = P(("grp", "blk", "node", "pair"), None)
    return jax.shard_map(
        per_device, mesh=mesh, in_specs=in_specs, out_specs=out_specs, check_vma=False
    )
```
